32 devices in a mesh: gx: 2 (over x), gy: 4 (over z), gz: 4 (over y, core).
Axes of the slice: x: 2, y: 2, z: 4, core: 2. Of those that a mesh axis runs over, the one named last changes fastest.
Arguments:
- offsets: float32 [3, 4, 8, 8, 128], P(None, 'gx', 'gy', 'gz'), may hold values from 0 to 1
- masses: float32 [4, 8, 8, 128], P('gx', 'gy', 'gz'), may hold values from 0.12 to 3
- smoothing: float32 [4, 8, 8, 128], P('gx', 'gy', 'gz'), may hold values from 0.6 to 0.75
- velocity: float32 [3, 4, 8, 8, 128], P(None, 'gx', 'gy', 'gz'), may hold values from -6 to 6
- energy: float32 [4, 8, 8, 128], P('gx', 'gy', 'gz'), may hold values from 0.3 to 3
- active: int32 [4, 8, 8, 128], P('gx', 'gy', 'gz'), may hold values from 0 to 1, as said below
Outputs:
- density: float32 [4, 8, 8, 128], P('gx', 'gy', 'gz')
- acceleration: float32 [3, 4, 8, 8, 128], P(None, 'gx', 'gy', 'gz')
- heating: float32 [4, 8, 8, 128], P('gx', 'gy', 'gz')
The draws below stay inside these ranges and needn't reach their ends.
Inputs may be any that keep to these rules, and one draw needn't show every extreme that they name: The share of active particles differs from cell to cell, from none to all.
All inputs are finite; a program needn't handle non-finite values.
Results may differ from the reference program's by a relative error of at most 0.0003.
Values sent between devices are 32-bit elements; how exact they have to be, the bound alone decides.
No kernel may reach another device: no remote copies, remote signals or barrier semaphores. Data moves between devices by JAX's collectives and lax.ppermute only.
A program may use at most 64 MiB of HBM per device.

```python
import math
import jax
import jax.numpy as jnp
from jax import lax

P_SIZE = 128
PASSES = 2
NCX = 4
NCY = 8
NCZ = 8


def draw_active(key, part):
    levels = jax.random.randint(jax.random.fold_in(key, 11), (NCX, NCY, NCZ, 1), 0, 9)
    tickets = jax.random.randint(jax.random.fold_in(key, 12), (NCX, NCY, NCZ, P_SIZE), 0, 8)
    return (tickets < levels).astype(jnp.int32)


def draw_masses(key, part):
    shape = (NCX, NCY, NCZ, P_SIZE)
    tickets = jax.random.randint(jax.random.fold_in(key, 21), shape, 0, 16)
    heavy = tickets == 0
    light_mass = jnp.exp(jax.random.uniform(jax.random.fold_in(key, 22), shape, jnp.float32, math.log(0.12), math.log(0.2)))
    heavy_mass = jnp.exp(jax.random.uniform(jax.random.fold_in(key, 23), shape, jnp.float32, math.log(2.4), math.log(3.0)))
    chosen = jnp.where(heavy, heavy_mass, light_mass)
    return jnp.clip(chosen, 0.12, 3.0).astype(jnp.float32)


def steps_of(stream_key, extent, cuts, least, top_value):
    def one(axis_at, shards_of):
        draws = jax.random.uniform(jax.random.fold_in(jax.random.fold_in(stream_key, 6), axis_at), (shards_of,), jnp.float32, least / len(cuts), top_value / len(cuts))
        return jnp.repeat(jnp.exp(draws), extent[axis_at] // shards_of).reshape((-1,) + (1,) * (len(extent) - axis_at - 1))

    level = one(*cuts[0])
    for cut in cuts[1:]:
        level = level * one(*cut)
    return level


def noise(own_key, extent, width, bound, split=(), held_as=jnp.bfloat16):
    drawn = jax.random.normal(own_key, extent, jnp.float32) * width
    if len(split) > 0:
        drawn = steps_of(own_key, extent, split, -0.22, 0.18) * drawn
    return jnp.clip(drawn, min=-bound, max=bound).astype(held_as)


def setup_inputs(seed: int = 0) -> dict:
    splits = jax.random.split(jax.random.key(seed), 7)
    return {
        "offsets": jnp.clip(1.0 * jax.random.uniform(splits[0], (3, NCX, NCY, NCZ, P_SIZE), jnp.float32) ** steps_of(splits[0], (3, NCX, NCY, NCZ, P_SIZE), ((1, 2), (2, 4), (3, 4)), -0.2, 0.2), 0.0, 1.0),
        "masses": draw_masses(jax.random.fold_in(splits[6], 71), 0),
        "smoothing": jnp.clip(0.6 + 0.14999998 * jax.random.uniform(splits[2], (NCX, NCY, NCZ, P_SIZE), jnp.float32) ** steps_of(splits[2], (NCX, NCY, NCZ, P_SIZE), ((0, 2), (1, 4), (2, 4)), -0.2, 0.2), 0.6, 0.75),
        "velocity": noise(splits[3], (3, NCX, NCY, NCZ, P_SIZE), 1.0, 6.0, ((1, 2), (2, 4), (3, 4)), jnp.float32),
        "energy": jnp.clip(jnp.exp(math.log(3.0) - 2.3025851 * jax.random.uniform(splits[4], (NCX, NCY, NCZ, P_SIZE), jnp.float32) ** steps_of(splits[4], (NCX, NCY, NCZ, P_SIZE), ((0, 2), (1, 4), (2, 4)), -0.2, 0.2)), 0.3, 3.0),
        "active": draw_active(jax.random.fold_in(splits[6], 71), 0),
    }


kernel_norm = 2.5464790894703255
eta_factor = 2.3
gamma_index = 5.0 / 3.0

def kernel(radius, length):
    scaled = radius / length
    remain = 1.0 - scaled
    inner_part = 1.0 - 6.0 * scaled * scaled + 6.0 * scaled * scaled * scaled
    outer_part = 2.0 * remain * remain * remain
    profile = jnp.where(scaled < 0.5, inner_part, jnp.where(scaled < 1.0, outer_part, 0.0))
    return kernel_norm * profile / (length * length * length)

def slope(radius, length):
    scaled = radius / length
    remain = 1.0 - scaled
    inner_part = 18.0 * scaled - 12.0
    outer_part = -6.0 * remain * remain / jnp.maximum(scaled, 0.5)
    profile = jnp.where(scaled < 0.5, inner_part, jnp.where(scaled < 1.0, outer_part, 0.0))
    square = length * length
    return kernel_norm * profile / (square * square * length)

def window(member, shift_x, shift_y, shift_z, count_y, count_z):
    return member[..., shift_x:shift_x + 1, shift_y:shift_y + count_y, shift_z:shift_z + count_z, :]

def separation(target_off, source_off, shift_x, shift_y, shift_z):
    count_y = target_off.shape[2]
    count_z = target_off.shape[3]
    source_slab = window(source_off, shift_x, shift_y, shift_z, count_y, count_z)
    deltas = []
    for component, offset_cell in enumerate((shift_x, shift_y, shift_z)):
        deltas.append(target_off[component][..., :, None] - source_slab[component][..., None, :] - (offset_cell - 1.0))
    radius = jnp.sqrt(deltas[0] * deltas[0] + deltas[1] * deltas[1] + deltas[2] * deltas[2])
    return (deltas, radius)

def density_slab(targets, sources):
    target_off, length = targets
    source_off, source_mass = sources
    count_y = length.shape[1]
    count_z = length.shape[2]
    summed = jnp.zeros(length.shape, jnp.float32)
    for shift_x in range(3):
        for shift_y in range(3):
            for shift_z in range(3):
                deltas, radius = separation(target_off, source_off, shift_x, shift_y, shift_z)
                weight = window(source_mass, shift_x, shift_y, shift_z, count_y, count_z)
                summed = summed + lax.optimization_barrier(jnp.sum(weight[..., None, :] * kernel(radius, length[..., None]), axis=-1))
    return (summed,)

def force_slab(targets, sources):
    target_off, length, density_now, veloc, energy_now = targets
    source_off, source_mass, source_len, source_dens, source_vel, source_energy = sources
    count_y = length.shape[1]
    count_z = length.shape[2]
    pressure = (gamma_index - 1.0) * energy_now / density_now
    source_press = (gamma_index - 1.0) * source_energy / source_dens
    pushes = [jnp.zeros(length.shape, jnp.float32) for component in range(3)]
    heating = jnp.zeros(length.shape, jnp.float32)
    for shift_x in range(3):
        for shift_y in range(3):
            for shift_z in range(3):
                deltas, radius = separation(target_off, source_off, shift_x, shift_y, shift_z)
                mass_j = window(source_mass, shift_x, shift_y, shift_z, count_y, count_z)[..., None, :]
                press_j = window(source_press, shift_x, shift_y, shift_z, count_y, count_z)[..., None, :]
                len_j = window(source_len, shift_x, shift_y, shift_z, count_y, count_z)[..., None, :]
                vel_j = window(source_vel, shift_x, shift_y, shift_z, count_y, count_z)
                own_slope = slope(radius, length[..., None])
                their_slope = slope(radius, len_j)
                coupling = mass_j * (pressure[..., None] * own_slope + press_j * their_slope)
                approach = deltas[0] * (veloc[0][..., :, None] - vel_j[0][..., None, :])
                approach = approach + deltas[1] * (veloc[1][..., :, None] - vel_j[1][..., None, :])
                approach = approach + deltas[2] * (veloc[2][..., :, None] - vel_j[2][..., None, :])
                heating = heating + lax.optimization_barrier(jnp.sum(mass_j * own_slope * approach, axis=-1))
                for component in range(3):
                    pushes[component] = pushes[component] - lax.optimization_barrier(jnp.sum(coupling * deltas[component], axis=-1))
    return (jnp.stack(pushes), pressure * heating)

def sweep(kernel_fn, targets, sources):
    count = targets[1].shape[0]

    def one_slab(first_slab):
        parts_t = tuple((lax.dynamic_slice_in_dim(member, first_slab, 1, member.ndim - 4) for member in targets))
        parts_s = tuple((lax.dynamic_slice_in_dim(member, first_slab, 3, member.ndim - 4) for member in sources))
        return kernel_fn(parts_t, parts_s)
    stacked = lax.map(one_slab, jnp.arange(count, dtype=jnp.int32))
    results = []
    for member in stacked:
        flat = jnp.squeeze(member, axis=member.ndim - 4)
        results.append(jnp.moveaxis(flat, 0, flat.ndim - 4))
    return tuple(results)

def settle(target_off, target_mass, length, source_off, source_mass):
    density_now = length
    for pass_index in range(PASSES):
        density_now, = sweep(density_slab, (target_off, length), (source_off, source_mass))
        length = eta_factor * jnp.cbrt(target_mass / density_now)
    return (length, density_now)

def wrap(field):
    widths = [(0, 0)] * (field.ndim - 4) + [(1, 1), (1, 1), (1, 1), (0, 0)]
    return jnp.pad(field, widths, mode='wrap')

def reference(offsets, masses, smoothing, velocity, energy, active):
    pad_off = wrap(offsets)
    pad_mass = wrap(masses)
    length, density_now = settle(offsets, masses, smoothing, pad_off, pad_mass)
    sources = (pad_off, pad_mass, wrap(length), wrap(density_now), wrap(velocity), wrap(energy))
    pushes, heating = sweep(force_slab, (offsets, length, density_now, velocity, energy), sources)
    active_weight = active.astype(jnp.float32)
    return (density_now, pushes * active_weight, heating * active_weight)
```

```python
import functools

import jax
import jax.numpy as jnp
from jax import lax
from jax.experimental import pallas as pl
from jax.experimental.pallas import tpu as pltpu
from jax.sharding import PartitionSpec as P

PASSES = 2

kernel_norm = 2.5464790894703255
eta_factor = 2.3
gamma_index = 5.0 / 3.0

ROWS = 32
TINY = 1e-12
AXES = ("gx", "gy", "gz")


def ring(axis, step):
    count = lax.axis_size(axis)
    return [(i, (i + step) % count) for i in range(count)]


def halo(block):
    for dim, axis in enumerate(AXES):
        size = block.shape[dim]
        if lax.axis_size(axis) == 2:
            other = lax.ppermute(block, axis, ring(axis, 1))
            low = lax.slice_in_dim(other, size - 1, size, axis=dim)
            high = lax.slice_in_dim(other, 0, 1, axis=dim)
        else:
            low = lax.ppermute(
                lax.slice_in_dim(block, size - 1, size, axis=dim), axis, ring(axis, 1)
            )
            high = lax.ppermute(lax.slice_in_dim(block, 0, 1, axis=dim), axis, ring(axis, -1))
        block = jnp.concatenate([low, block, high], axis=dim)
    return block


def cube_root(value):
    return jnp.exp(jnp.log(value) * (1.0 / 3.0))


def split3(value):
    high = value.astype(jnp.bfloat16).astype(jnp.float32)
    rest = value - high
    mid = rest.astype(jnp.bfloat16).astype(jnp.float32)
    return high, mid, rest - mid


def row_index():
    return lax.broadcasted_iota(jnp.int32, (8, 128), 0)


def place(fields, origin):
    row = row_index()
    shift = jnp.where(row == 0, origin[0], jnp.where(row == 1, origin[1], origin[2]))
    spot = jnp.where(row < 3, fields + shift, 0.0)
    return spot, jnp.sum(spot * spot, axis=0, keepdims=True)


def source_rows(spot, square, scale):
    row = row_index()
    value = jnp.where(row == 3, square, jnp.where(row == 4, 1.0, spot)) * scale
    high, mid, low = split3(value)
    return jnp.concatenate([high, mid, high, mid, low, high], axis=0)


def target_rows(spot, square, scale):
    row = row_index()
    value = jnp.where(row == 3, 1.0, jnp.where(row == 4, square, -2.0 * spot)) * scale
    high, mid, low = split3(value)
    return jnp.concatenate([high, high, mid, mid, high, low], axis=0)


def weights_of(value):
    high, mid, low = split3(value)
    rows = jnp.concatenate([high, mid, low, jnp.zeros_like(low)], axis=0)
    return jnp.concatenate([rows, rows], axis=1).astype(jnp.bfloat16)


def product(left, right):
    return jnp.dot(left, right, preferred_element_type=jnp.float32)


def tiled(rows, count):
    return jnp.concatenate([rows] * count, axis=0)


def origin_of(cell, sizes):
    return [c - 0.5 * n for c, n in zip(cell, sizes)]


def cells_of(sizes):
    return [(x, y, z) for x in range(sizes[0]) for y in range(sizes[1]) for z in range(sizes[2])]


def density_kernel(src_ref, len_ref, rho_ref, r_ref, c_ref, *, sizes):
    nx, ny, nz = sizes
    cx, cy, cz = nx - 2, ny - 2, nz - 2
    for x, y, z in cells_of(sizes):
        fields = src_ref[x, y, z]
        spot, square = place(fields, origin_of((x, y, z), sizes))
        root = cube_root(fields[3:4])
        r_ref[x * ny + y, :, z * 128 : (z + 1) * 128] = source_rows(
            spot, square, root * root
        ).astype(jnp.bfloat16)
        c_ref[x * ny + y, :, z * 128 : (z + 1) * 128] = jnp.broadcast_to(root, (8, 128))

    def one_cell(index, carry):
        x = index // (cy * cz)
        y = index // cz % cy
        z = index % cz
        fields = src_ref[x + 1, y + 1, z + 1]
        where = [v.astype(jnp.float32) + (1.0 - 0.5 * n) for v, n in zip((x, y, z), sizes)]
        spot, square = place(fields, where)
        length = len_ref[x, y, pl.ds(z, 1), :]
        lanes = pl.ds(pl.multiple_of(z * 128, 128), 384)
        for pass_index in range(PASSES):
            inverse = 1.0 / length
            left = target_rows(spot, square, inverse * inverse).T.astype(jnp.bfloat16)
            sums = []
            for first in range(0, 128, ROWS):
                near = jnp.zeros((ROWS, 128), jnp.float32)
                far = jnp.zeros((ROWS, 128), jnp.float32)
                for dx in range(3):
                    for dy in range(3):
                        line = (x + dx) * ny + y + dy
                        s = product(left[first : first + ROWS], r_ref[line, :, lanes])
                        root = tiled(c_ref[line, :, lanes], ROWS // 8)
                        s = jnp.maximum(s, TINY)
                        scaled = s * lax.rsqrt(s)
                        t = root - scaled
                        a = jnp.maximum(t, 0.0)
                        b = jnp.maximum(t - scaled, 0.0)
                        a = a * a * a
                        b = b * b * b
                        for k in range(3):
                            far = far + a[:, k * 128 : (k + 1) * 128]
                            near = near + b[:, k * 128 : (k + 1) * 128]
                sums.append(2.0 * far - near)
            total = jnp.sum(jnp.concatenate(sums, axis=0).T, axis=0, keepdims=True)
            density = kernel_norm * total * (inverse * inverse * inverse)
            length = eta_factor * cube_root(fields[3:4] / density)
        rho_ref[x, y, pl.ds(z, 1), :] = density
        return carry

    lax.fori_loop(0, cx * cy * cz, one_cell, 0)


def profile(s):
    s = jnp.maximum(s, TINY)
    rs = lax.rsqrt(s)
    q = s * rs
    t = 1.0 - q
    a = jnp.maximum(t, 0.0)
    b = jnp.maximum(t - q, 0.0)
    g = jnp.minimum(a, q) * (a + b) * rs
    high = g.astype(jnp.bfloat16)
    low = (g - high.astype(jnp.float32)).astype(jnp.bfloat16)
    return jnp.concatenate([high, low], axis=0)


def own_basis(fields, spot):
    row = row_index()
    along = jnp.sum(fields[4:7] * spot[0:3], axis=0, keepdims=True)
    basis = jnp.where(row < 3, spot, jnp.where(row == 3, 1.0, fields))
    return jnp.where(row == 7, along, basis)


def smooth(fields, density):
    inverse = 1.0 / (eta_factor * cube_root(fields[3:4] / density))
    inv2 = inverse * inverse
    press = (gamma_index - 1.0) * fields[7:8] / density
    return inv2, press * (-6.0 * kernel_norm) * inv2 * inv2 * inverse


def gather_sums(right, point_ref, col_ref, x, y, z, ny):
    total = jnp.zeros((32, 128), jnp.float32)
    for dx in range(3):
        for dy in range(3):
            line = (x + dx) * ny + y + dy
            for dz in range(3):
                rows = pl.ds(pl.multiple_of((z + dz) * 128, 128), 128)
                lanes = pl.ds(pl.multiple_of((z + dz) * 256, 256), 256)
                g = profile(product(point_ref[line, rows, :], right))
                total = total + product(col_ref[line, :, lanes], g)
    return total[0:8] + total[8:16] + total[16:24]


def target_place(src_ref, x, y, z, sizes):
    fields = src_ref[x + 1, y + 1, z + 1]
    where = [v.astype(jnp.float32) + (1.0 - 0.5 * n) for v, n in zip((x, y, z), sizes)]
    spot, square = place(fields, where)
    return fields, spot, square


def own_kernel(src_ref, rho_ref, sum_ref, point_ref, col_ref, *, sizes):
    nx, ny, nz = sizes
    cx, cy, cz = nx - 2, ny - 2, nz - 2
    for x, y, z in cells_of(sizes):
        fields = src_ref[x, y, z]
        spot, square = place(fields, origin_of((x, y, z), sizes))
        line = x * ny + y
        point_ref[line, z * 128 : (z + 1) * 128, :] = source_rows(spot, square, 1.0).T.astype(
            jnp.bfloat16
        )
        col_ref[line, :, z * 256 : (z + 1) * 256] = weights_of(
            own_basis(fields, spot) * fields[3:4]
        )

    def one_cell(index, carry):
        x = index // (cy * cz)
        y = index // cz % cy
        z = index % cz
        fields, spot, square = target_place(src_ref, x, y, z, sizes)
        inv2, strength = smooth(fields, rho_ref[x, y, pl.ds(z, 1), :])
        right = target_rows(spot, square, inv2).astype(jnp.bfloat16)
        sum_ref[x, y, z] = gather_sums(right, point_ref, col_ref, x, y, z, ny) * strength
        return carry

    lax.fori_loop(0, cx * cy * cz, one_cell, 0)


def their_kernel(
    src_ref, rho_ref, sum_ref, act_ref, push_ref, heat_ref, point_ref, col_ref, *, sizes
):
    nx, ny, nz = sizes
    cx, cy, cz = nx - 2, ny - 2, nz - 2
    row = row_index()
    for x, y, z in cells_of(sizes):
        fields = src_ref[x, y, z]
        spot, square = place(fields, origin_of((x, y, z), sizes))
        inv2, strength = smooth(fields, rho_ref[x, y, z])
        line = x * ny + y
        point_ref[line, z * 128 : (z + 1) * 128, :] = source_rows(spot, square, inv2).T.astype(
            jnp.bfloat16
        )
        basis = jnp.where(row == 3, 1.0, spot)
        col_ref[line, :, z * 256 : (z + 1) * 256] = weights_of(basis * (fields[3:4] * strength))

    def one_cell(index, carry):
        x = index // (cy * cz)
        y = index // cz % cy
        z = index % cz
        fields, spot, square = target_place(src_ref, x, y, z, sizes)
        right = target_rows(spot, square, 1.0).astype(jnp.bfloat16)
        their = gather_sums(right, point_ref, col_ref, x, y, z, ny)
        own = sum_ref[x, y, z]
        active = act_ref[x, y, pl.ds(z, 1), :].astype(jnp.float32)
        spot = spot[0:3]
        push = spot * (own[3:4] + their[3:4]) - own[0:3] - their[0:3]
        heat = fields[4:7] * (spot * own[3:4] - own[0:3]) - spot * own[4:7]
        heat = jnp.sum(heat, axis=0, keepdims=True) + own[7:8]
        for k in range(3):
            push_ref[k, x, y, pl.ds(z, 1), :] = -active * push[k : k + 1]
        heat_ref[x, y, pl.ds(z, 1), :] = active * heat
        return carry

    lax.fori_loop(0, cx * cy * cz, one_cell, 0)


def body(offsets, masses, smoothing, velocity, energy, active):
    local = masses.shape[:3]
    sizes = tuple(n + 2 for n in local)
    nx, ny, nz = sizes
    f32 = jnp.float32
    static = jnp.stack(
        [offsets[0], offsets[1], offsets[2], masses, velocity[0], velocity[1], velocity[2], energy],
        axis=3,
    )
    padded = halo(static)
    density = pl.pallas_call(
        functools.partial(density_kernel, sizes=sizes),
        out_shape=jax.ShapeDtypeStruct(masses.shape, f32),
        scratch_shapes=[
            pltpu.VMEM((nx * ny, 48, nz * 128), jnp.bfloat16),
            pltpu.VMEM((nx * ny, 8, nz * 128), f32),
        ],
        name="density",
    )(padded, smoothing)
    imported = halo(density[..., None, :])
    tables = [
        pltpu.VMEM((nx * ny, nz * 128, 48), jnp.bfloat16),
        pltpu.VMEM((nx * ny, 32, nz * 256), jnp.bfloat16),
    ]
    sums = pl.pallas_call(
        functools.partial(own_kernel, sizes=sizes),
        out_shape=jax.ShapeDtypeStruct(static.shape, f32),
        scratch_shapes=tables,
        name="own",
    )(padded, density)
    push, heat = pl.pallas_call(
        functools.partial(their_kernel, sizes=sizes),
        out_shape=(
            jax.ShapeDtypeStruct((3,) + masses.shape, f32),
            jax.ShapeDtypeStruct(masses.shape, f32),
        ),
        scratch_shapes=tables,
        name="their",
    )(padded, imported, sums, active)
    return (density, push, heat)


def solution(mesh):
    vector = P(None, "gx", "gy", "gz", None)
    scalar = P("gx", "gy", "gz", None)
    return jax.shard_map(
        body,
        mesh=mesh,
        in_specs=(vector, scalar, scalar, vector, scalar, scalar),
        out_specs=(scalar, vector, scalar),
        check_vma=False,
    )
```

```python
import functools

import jax
import jax.numpy as jnp
from jax import lax
from jax.experimental import pallas as pl
from jax.experimental.pallas import tpu as pltpu
from jax.sharding import PartitionSpec as P

PASSES = 2

kernel_norm = 2.5464790894703255
eta_factor = 2.3
gamma_index = 5.0 / 3.0

ROWS = 32
TINY = 1e-12
VMEM_LIMIT = 24 * 1024 * 1024
AXES = ("gx", "gy", "gz")


def ring(axis, step):
    count = lax.axis_size(axis)
    return [(i, (i + step) % count) for i in range(count)]


def halo(block):
    for dim, axis in enumerate(AXES):
        size = block.shape[dim]
        if lax.axis_size(axis) == 2:
            other = lax.ppermute(block, axis, ring(axis, 1))
            low = lax.slice_in_dim(other, size - 1, size, axis=dim)
            high = lax.slice_in_dim(other, 0, 1, axis=dim)
        else:
            low = lax.ppermute(
                lax.slice_in_dim(block, size - 1, size, axis=dim), axis, ring(axis, 1)
            )
            high = lax.ppermute(lax.slice_in_dim(block, 0, 1, axis=dim), axis, ring(axis, -1))
        block = jnp.concatenate([low, block, high], axis=dim)
    return block


def cube_root(value):
    return jnp.exp(jnp.log(value) * (1.0 / 3.0))


def split3(value):
    high = value.astype(jnp.bfloat16).astype(jnp.float32)
    rest = value - high
    mid = rest.astype(jnp.bfloat16).astype(jnp.float32)
    return high, mid, rest - mid


def row_index():
    return lax.broadcasted_iota(jnp.int32, (8, 128), 0)


def place(fields, origin):
    row = row_index()
    shift = jnp.where(row == 0, origin[0], jnp.where(row == 1, origin[1], origin[2]))
    spot = jnp.where(row < 3, fields + shift, 0.0)
    return spot, jnp.sum(spot * spot, axis=0, keepdims=True)


def source_rows(spot, square, scale):
    row = row_index()
    value = jnp.where(row == 3, square, jnp.where(row == 4, 1.0, spot)) * scale
    high, mid, low = split3(value)
    return jnp.concatenate([high, mid, high, mid, low, high], axis=0)


def target_rows(spot, square, scale):
    row = row_index()
    value = jnp.where(row == 3, 1.0, jnp.where(row == 4, square, -2.0 * spot)) * scale
    high, mid, low = split3(value)
    return jnp.concatenate([high, high, mid, mid, high, low], axis=0)


def product(left, right):
    return jnp.dot(left, right, preferred_element_type=jnp.float32)


def product_nt(left, right):
    return lax.dot_general(
        left, right, (((1,), (1,)), ((), ())), preferred_element_type=jnp.float32
    )


def product_tn(left, right):
    return lax.dot_general(
        left, right, (((0,), (0,)), ((), ())), preferred_element_type=jnp.float32
    )


def tiled(rows, count):
    return jnp.concatenate([rows] * count, axis=0)


def origin_of(cell, sizes):
    return [c - 0.5 * n for c, n in zip(cell, sizes)]


def cells_of(sizes):
    return [(x, y, z) for x in range(sizes[0]) for y in range(sizes[1]) for z in range(sizes[2])]


def half_up(count):
    return jnp.floor((count + 1.0) * 0.5)


def sort_kernel(src_ref, side_ref, *, local):
    row = row_index()
    across = lax.broadcasted_iota(jnp.int32, (128, 128), 0)
    along = lax.broadcasted_iota(jnp.int32, (128, 128), 1)
    earlier = across < along

    def rank(key):
        left = jnp.broadcast_to(key, (8, 128)).T[:, 0:1]
        ahead = (left < key) | (earlier & (left == key))
        return jnp.sum(jnp.where(ahead, 1.0, 0.0), axis=0, keepdims=True)

    for index, cell in enumerate(cells_of(local)):
        fields = src_ref[cell]
        mass = fields[3:4]
        heavy = jnp.where(mass > jnp.sum(mass, axis=1, keepdims=True) * (1.0 / 128.0), 1.0, 0.0)
        light = 128.0 - jnp.sum(heavy, axis=1, keepdims=True)
        base = jnp.zeros((1, 128), jnp.float32)
        size = jnp.broadcast_to(light, (1, 128))
        group = jnp.zeros((1, 128), jnp.float32)
        bits = []
        for dim in range(3):
            place_in = rank(fields[dim : dim + 1] + 2.0 * group + 64.0 * heavy) - base
            first = half_up(size)
            bit = jnp.where(place_in >= first, 1.0, 0.0) * (1.0 - heavy)
            base = base + bit * first
            size = jnp.where(bit > 0.0, size - first, first)
            group = 2.0 * group + bit
            place_in = place_in - bit * first
            bits.append(bit)
        slot = jnp.where(heavy > 0.0, -1.0, 16.0 * group + place_in)
        side = jnp.where(row == 0, bits[0], jnp.where(row == 1, bits[1], bits[2]))
        side = jnp.where(row == 3, heavy, side)
        side_ref[index] = jnp.where(row == 4, slot, side)


def halves_of(source, count):
    reach = []
    for half in range(2 * count):
        cell = half // 2 + 1
        if source in ((cell - 1, cell) if half % 2 == 0 else (cell, cell + 1)):
            reach.append(half)
    return reach


def near_of(source, count):
    return [c for c in range(count) if abs(c + 1 - source) <= 1]


def runs_of(ranges, counts):
    xs, ys, zs = ranges
    return [
        (((x * counts[1] + y) * counts[2] + zs[0]) * 16, len(zs) * 16) for x in xs for y in ys
    ]


def main_kernel(
    src_ref,
    len_ref,
    side_ref,
    act_ref,
    rho_ref,
    push_ref,
    heat_ref,
    out_ref,
    dens_ref,
    root_ref,
    flat_ref,
    col_ref,
    size_ref,
    left_ref,
    feat_ref,
    oct_ref,
    rest_ref,
    far_ref,
    close_ref,
    own_ref,
    their_ref,
    sum_ref,
    count_ref,
    *,
    sizes,
):
    nx, ny, nz = sizes
    local = cx, cy, cz = nx - 2, ny - 2, nz - 2
    halves = (2 * cx, 2 * cy, 2 * cz)
    cells = cells_of(local)
    inner = len(cells) * 128
    row = row_index()
    across = lax.broadcasted_iota(jnp.int32, (128, 128), 0)
    along = lax.broadcasted_iota(jnp.int32, (128, 128), 1)
    before = jnp.where(across < along, 1.0, 0.0).astype(jnp.bfloat16)
    slot_of = across.astype(jnp.float32)
    first16 = lax.broadcasted_iota(jnp.int32, (16, 128), 0).astype(jnp.float32)

    for x, y, z in cells_of(sizes):
        fields = src_ref[x, y, z]
        spot, square = place(fields, origin_of((x, y, z), sizes))
        mass = fields[3:4]
        root = cube_root(mass)
        line = x * ny + y
        part = slice(z * 128, (z + 1) * 128)
        dens_ref[line, :, part] = source_rows(spot, square, root * root).astype(jnp.bfloat16)
        flat_ref[line, :, part] = source_rows(spot, square, 1.0).astype(jnp.bfloat16)
        root_ref[line, :, part] = jnp.broadcast_to(root, (8, 128))
        moving = jnp.sum(fields[4:7] * spot[0:3], axis=0, keepdims=True)
        basis = jnp.where(row < 3, spot, jnp.where(row == 3, 1.0, fields))
        basis = jnp.where(row == 7, moving, basis) * mass
        cols = jnp.concatenate(split3(basis), axis=0).T.astype(jnp.bfloat16)
        col_ref[line, z * 256 : z * 256 + 128, :] = cols
        col_ref[line, z * 256 + 128 : z * 256 + 256, :] = cols

    def spline(s, root):
        s = jnp.maximum(s, TINY)
        scaled = s * lax.rsqrt(s)
        t = root - scaled
        a = jnp.maximum(t, 0.0)
        b = jnp.maximum(t - scaled, 0.0)
        return a * a * a, b * b * b

    def dense_sums(left, x, y, z):
        count = left.shape[0]
        near = jnp.zeros((count, 128), jnp.float32)
        far = jnp.zeros((count, 128), jnp.float32)
        lanes = pl.ds(pl.multiple_of(z * 128, 128), 384)
        for dx in range(3):
            for dy in range(3):
                line = (x + dx) * ny + y + dy
                s = product(left, dens_ref[line, :, lanes])
                a, b = spline(s, tiled(root_ref[line, :, lanes], count // 8))
                for k in range(3):
                    far = far + a[:, k * 128 : (k + 1) * 128]
                    near = near + b[:, k * 128 : (k + 1) * 128]
        return 2.0 * far - near

    def first_pass(index, carry):
        x = index // (cy * cz)
        y = index // cz % cy
        z = index % cz
        fields = src_ref[x + 1, y + 1, z + 1]
        where = [v.astype(jnp.float32) + (1.0 - 0.5 * n) for v, n in zip((x, y, z), sizes)]
        spot, square = place(fields, where)
        inverse = 1.0 / len_ref[x, y, pl.ds(z, 1), :]
        left = target_rows(spot, square, inverse * inverse).T.astype(jnp.bfloat16)
        sums = [dense_sums(left[k : k + ROWS], x, y, z) for k in range(0, 128, ROWS)]
        total = jnp.sum(jnp.concatenate(sums, axis=0).T, axis=0, keepdims=True)
        density = kernel_norm * total * (inverse * inverse * inverse)
        length = eta_factor * cube_root(fields[3:4] / density)
        size_ref[index] = jnp.broadcast_to(length, (8, 128))
        return carry

    lax.fori_loop(0, cx * cy * cz, first_pass, 0)

    def cell_runs(cell):
        x, y, z = cell
        return [
            (((2 * x + bx) * halves[1] + 2 * y + by) * halves[2] + 2 * z) * 16
            for bx in range(2)
            for by in range(2)
        ]

    def scatter_rows(ref, index, cell, value):
        for k, start in enumerate(cell_runs(cell)):
            ref[start : start + 32, :] = value[k * 32 : (k + 1) * 32]

    def gather_rows(value_of, cell):
        return jnp.concatenate([value_of(start) for start in cell_runs(cell)], axis=0)

    def choose(index, fields, length):
        side = side_ref[index]
        reach = jnp.where(side > 0.0, length - fields, fields + length - 1.0)
        wide = jnp.where((row < 3) & (reach > 0.0), 1.0, 0.0)
        wide = jnp.where(row == 3, side, wide)
        wide = jnp.max(wide, axis=0, keepdims=True)
        order = product(jnp.broadcast_to(wide, (8, 128)).astype(jnp.bfloat16), before)[0:1]
        order = jnp.where(wide > 0.0, order, -1.0)
        count_ref[index] = jnp.sum(wide).astype(jnp.int32)
        slot = jnp.where(wide > 0.0, -1.0, side[4:5])
        oct_ref[index] = jnp.where(slot_of == slot, 1.0, 0.0).astype(jnp.bfloat16)
        rest_ref[index] = jnp.broadcast_to(order, (8, 128))
        return picked(index, 0)

    def picked(index, chunk):
        order = rest_ref[index][0:1]
        shift = jnp.float32(16.0) * chunk
        return jnp.where(first16 + shift == order, 1.0, 0.0)

    def set_rows(index, cell, fields, spot, square, length, weight):
        inverse = 1.0 / length
        rest = choose(index, fields, length).astype(jnp.bfloat16)
        left = target_rows(spot, square, inverse * inverse).astype(jnp.bfloat16)
        chosen = oct_ref[index]
        scatter_rows(left_ref, index, cell, product_nt(chosen, left).astype(jnp.bfloat16))
        part = slice(inner + index * 16, inner + index * 16 + 16)
        left_ref[part, :] = product_nt(rest, left).astype(jnp.bfloat16)
        if weight is not None:
            feat = jnp.concatenate(split3(weight), axis=0).astype(jnp.bfloat16)
            scatter_rows(feat_ref, index, cell, product_nt(chosen, feat).astype(jnp.bfloat16))
            feat_ref[part, :] = product_nt(rest, feat).astype(jnp.bfloat16)

    def source_runs(x, y, z):
        ranges = [halves_of(s, n) for s, n in zip((x, y, z), local)]
        runs = runs_of(ranges, halves)
        ranges = [near_of(s, n) for s, n in zip((x, y, z), local)]
        return runs + [(inner + start, size) for start, size in runs_of(ranges, local)]

    def rows_of(ref, runs):
        return jnp.concatenate([ref[start : start + size, :] for start, size in runs], axis=0)

    def add_rows(ref, runs, value):
        at = 0
        for start, size in runs:
            ref[start : start + size, :] += value[at : at + size]
            at += size

    def unsorted_column(index, octant, rest):
        total = jnp.sum(octant, axis=1, keepdims=True) * oct_ref[index].astype(jnp.float32)
        total = jnp.sum(total, axis=0, keepdims=True)
        rest = jnp.sum(rest, axis=1, keepdims=True) * picked(index, 0)
        return total + jnp.sum(rest, axis=0, keepdims=True)

    def extras(visit):
        def one_cell(index, carry):
            def one_chunk(chunk, carry):
                x = index // (cy * cz)
                y = index // cz % cy
                z = index % cz
                fields = src_ref[x + 1, y + 1, z + 1]
                where = [v.astype(jnp.float32) + (1.0 - 0.5 * n) for v, n in zip((x, y, z), sizes)]
                spot, square = place(fields, where)
                inverse = 1.0 / size_ref[index][0:1]
                rest = picked(index, chunk.astype(jnp.float32))
                left = target_rows(spot, square, inverse * inverse).astype(jnp.bfloat16)
                left = product_nt(rest.astype(jnp.bfloat16), left).astype(jnp.bfloat16)
                visit(index, (x, y, z), fields, spot, rest, left)
                return carry

            return lax.fori_loop(1, (count_ref[index] + 15) // 16, one_chunk, carry)

        lax.fori_loop(0, cx * cy * cz, one_cell, 0)

    def weight_of(fields, spot, strength):
        return jnp.where(row < 3, spot, jnp.where(row == 3, 1.0, 0.0)) * (fields[3:4] * strength)

    def extra_density(index, cell, fields, spot, rest, left):
        extra = jnp.sum(dense_sums(left, *cell), axis=1, keepdims=True) * rest
        sum_ref[index, 0:8, :] += jnp.sum(extra, axis=0, keepdims=True)

    def unsort(value, rest):
        pieces = split3(value)
        rest = rest.astype(jnp.bfloat16)
        total = product_tn(pieces[0].astype(jnp.bfloat16), rest)
        total += product_tn(pieces[1].astype(jnp.bfloat16), rest)
        return total + product_tn(pieces[2].astype(jnp.bfloat16), rest)

    def extra_force(index, cell, fields, spot, rest, left):
        x, y, z = cell
        feat = jnp.concatenate(split3(weight_of(fields, spot, size_ref[index][1:2])), axis=0)
        feat = product_nt(rest.astype(jnp.bfloat16), feat.astype(jnp.bfloat16))
        feat = feat.astype(jnp.bfloat16)
        total = jnp.zeros((16, 24), jnp.float32)
        for dx in range(3):
            for dy in range(3):
                line = (x + dx) * ny + y + dy
                lanes = pl.ds(pl.multiple_of(z * 128, 128), 384)
                high, low = profile(product(left, flat_ref[line, :, lanes]))
                for dz in range(3):
                    cols = col_ref[line, pl.ds(pl.multiple_of((z + dz) * 256, 256), 256), :]
                    part = slice(dz * 128, (dz + 1) * 128)
                    pair = jnp.concatenate([high[:, part], low[:, part]], axis=1)
                    total += product(pair, cols)
                their_ref[line, :, lanes] += product_tn(feat, high) + product_tn(feat, low)
        sum_ref[index] += unsort(total, rest)

    placed = []
    for index, cell in enumerate(cells):
        fields = src_ref[cell[0] + 1, cell[1] + 1, cell[2] + 1]
        origin = origin_of([c + 1 for c in cell], sizes)
        placed.append((fields, origin))
        spot, square = place(fields, origin)
        set_rows(index, cell, fields, spot, square, size_ref[index][0:1], None)

    far_ref[...] = jnp.zeros_like(far_ref)
    close_ref[...] = jnp.zeros_like(close_ref)
    for x, y, z in cells_of(sizes):
        runs = source_runs(x, y, z)
        line = x * ny + y
        part = slice(z * 128, (z + 1) * 128)
        left = rows_of(left_ref, runs)
        s = product(left, dens_ref[line, :, part])
        a, b = spline(s, tiled(root_ref[line, :, part], left.shape[0] // 8))
        add_rows(far_ref, runs, a)
        add_rows(close_ref, runs, b)

    for index, cell in enumerate(cells):
        part = slice(inner + index * 16, inner + index * 16 + 16)
        octant = gather_rows(
            lambda start: 2.0 * far_ref[start : start + 32, :] - close_ref[start : start + 32, :],
            cell,
        )
        total = unsorted_column(index, octant, 2.0 * far_ref[part, :] - close_ref[part, :])
        sum_ref[index, 0:8, :] = jnp.broadcast_to(total, (8, 128))
    extras(extra_density)
    for index, cell in enumerate(cells):
        x, y, z = cell
        fields, origin = placed[index]
        spot, square = place(fields, origin)
        inverse = 1.0 / size_ref[index][0:1]
        density = kernel_norm * sum_ref[index, 0:1, :] * (inverse * inverse * inverse)
        rho_ref[x, y, z : z + 1, :] = density
        length = eta_factor * cube_root(fields[3:4] / density)
        inv2, strength = smooth(fields, density)
        size_ref[index] = jnp.where(row == 0, length, strength)
        set_rows(index, cell, fields, spot, square, length, weight_of(fields, spot, strength))

    own_ref[...] = jnp.zeros_like(own_ref)

    def slopes(x, y, z):
        runs = source_runs(x, y, z)
        line = x * ny + y
        part = slice(z * 128, (z + 1) * 128)
        high, low = profile(product(rows_of(left_ref, runs), flat_ref[line, :, part]))
        return line, z, runs, high, low

    def sums(line, z, runs, high, low):
        part = slice(z * 128, (z + 1) * 128)
        cols = col_ref[line, z * 256 : (z + 1) * 256, :]
        add_rows(own_ref, runs, product(jnp.concatenate([high, low], axis=1), cols))
        feat = rows_of(feat_ref, runs)
        their_ref[line, :, part] = product_tn(feat, high) + product_tn(feat, low)

    waiting = None
    for source in cells_of(sizes):
        ready = slopes(*source)
        if waiting is not None:
            sums(*waiting)
        waiting = ready
    sums(*waiting)

    for index, cell in enumerate(cells):
        octant = gather_rows(lambda start: own_ref[start : start + 32, :], cell)
        part = slice(inner + index * 16, inner + index * 16 + 16)
        own = unsort(octant, oct_ref[index]) + unsort(own_ref[part, :], picked(index, 0))
        sum_ref[index] = own
    extras(extra_force)
    for index, cell in enumerate(cells):
        x, y, z = cell
        fields, origin = placed[index]
        spot, square = place(fields, origin)
        own = sum_ref[index]
        own = (own[0:8] + own[8:16] + own[16:24]) * size_ref[index][1:2]
        active = act_ref[x, y, z : z + 1, :].astype(jnp.float32)
        spot = spot[0:3]
        push = spot * own[3:4] - own[0:3]
        heat = fields[4:7] * push - spot * own[4:7]
        heat = jnp.sum(heat, axis=0, keepdims=True) + own[7:8]
        push_ref[x, y, z] = jnp.concatenate([push, active], axis=0)
        heat_ref[x, y, z : z + 1, :] = active * heat

    for x, y, z in cells_of(sizes):
        spot, square = place(src_ref[x, y, z], origin_of((x, y, z), sizes))
        their = their_ref[x * ny + y, :, z * 128 : (z + 1) * 128]
        their = their[0:8] + their[8:16] + their[16:24]
        out_ref[x, y, z] = (spot * their[3:4] - their)[0:4]


def profile(s):
    s = jnp.maximum(s, TINY)
    rs = lax.rsqrt(s)
    q = s * rs
    t = 1.0 - q
    a = jnp.maximum(t, 0.0)
    b = jnp.maximum(t - q, 0.0)
    g = jnp.minimum(a, q) * (a + b) * rs
    high = g.astype(jnp.bfloat16)
    return high, (g - high.astype(jnp.float32)).astype(jnp.bfloat16)


def smooth(fields, density):
    inverse = 1.0 / (eta_factor * cube_root(fields[3:4] / density))
    inv2 = inverse * inverse
    press = (gamma_index - 1.0) * fields[7:8] / density
    return inv2, press * (-6.0 * kernel_norm) * inv2 * inv2 * inverse


def take(block, dim, start, stop):
    return lax.slice_in_dim(block, start, stop, axis=dim)


def fold(block):
    for dim in (2, 1, 0):
        axis = AXES[dim]
        last = block.shape[dim] - 1
        low, high = take(block, dim, 0, 1), take(block, dim, last, last + 1)
        if lax.axis_size(axis) == 2:
            both = lax.ppermute(jnp.concatenate([high, low], axis=dim), axis, ring(axis, 1))
            to_first, to_last = take(both, dim, 0, 1), take(both, dim, 1, 2)
        else:
            to_last = lax.ppermute(low, axis, ring(axis, -1))
            to_first = lax.ppermute(high, axis, ring(axis, 1))
        block = take(block, dim, 1, last)
        count = last - 1
        if count == 1:
            block = block + to_first + to_last
        else:
            block = jnp.concatenate(
                [
                    take(block, dim, 0, 1) + to_first,
                    take(block, dim, 1, count - 1),
                    take(block, dim, count - 1, count) + to_last,
                ],
                axis=dim,
            )
    return block


def body(offsets, masses, smoothing, velocity, energy, active):
    local = masses.shape[:3]
    sizes = tuple(n + 2 for n in local)
    nx, ny, nz = sizes
    f32 = jnp.float32
    bf16 = jnp.bfloat16
    ncell = local[0] * local[1] * local[2]
    static = jnp.stack(
        [offsets[0], offsets[1], offsets[2], masses, velocity[0], velocity[1], velocity[2], energy],
        axis=3,
    )
    side = pl.pallas_call(
        functools.partial(sort_kernel, local=local),
        out_shape=jax.ShapeDtypeStruct((ncell, 8, 128), f32),
        compiler_params=pltpu.CompilerParams(vmem_limit_bytes=VMEM_LIMIT),
        name="sort",
    )(static)
    padded = halo(static)
    lines = nx * ny
    rows = ncell * 144
    density, push, heat, spread = pl.pallas_call(
        functools.partial(main_kernel, sizes=sizes),
        out_shape=(
            jax.ShapeDtypeStruct(masses.shape, f32),
            jax.ShapeDtypeStruct(local + (4, 128), f32),
            jax.ShapeDtypeStruct(masses.shape, f32),
            jax.ShapeDtypeStruct(sizes + (4, 128), f32),
        ),
        scratch_shapes=[
            pltpu.VMEM((lines, 48, nz * 128), bf16),
            pltpu.VMEM((lines, 8, nz * 128), f32),
            pltpu.VMEM((lines, 48, nz * 128), bf16),
            pltpu.VMEM((lines, nz * 256, 24), bf16),
            pltpu.VMEM((ncell, 8, 128), f32),
            pltpu.VMEM((rows, 48), bf16),
            pltpu.VMEM((rows, 24), bf16),
            pltpu.VMEM((ncell, 128, 128), bf16),
            pltpu.VMEM((ncell, 8, 128), f32),
            pltpu.VMEM((rows, 128), f32),
            pltpu.VMEM((rows, 128), f32),
            pltpu.VMEM((rows, 24), f32),
            pltpu.VMEM((lines, 24, nz * 128), f32),
            pltpu.VMEM((ncell, 24, 128), f32),
            pltpu.SMEM((ncell,), jnp.int32),
        ],
        compiler_params=pltpu.CompilerParams(vmem_limit_bytes=VMEM_LIMIT),
        name="main",
    )(padded, smoothing, side, active)
    total = -(push[..., 0:3, :] + fold(spread)[..., 0:3, :]) * push[..., 3:4, :]
    return (density, jnp.moveaxis(total, 3, 0), heat)


def solution(mesh):
    vector = P(None, "gx", "gy", "gz", None)
    scalar = P("gx", "gy", "gz", None)
    return jax.shard_map(
        body,
        mesh=mesh,
        in_specs=(vector, scalar, scalar, vector, scalar, scalar),
        out_specs=(scalar, vector, scalar),
        check_vma=False,
    )
```

```python
import functools

import jax
import jax.numpy as jnp
from jax import lax
from jax.experimental import pallas as pl
from jax.experimental.pallas import tpu as pltpu
from jax.sharding import PartitionSpec as P


kernel_norm = 2.5464790894703255
eta_factor = 2.3
gamma_index = 5.0 / 3.0

ROWS = 32
TINY = 1e-12
WIDE = 32
VMEM_LIMIT = 24 * 1024 * 1024
AXES = ("gx", "gy", "gz")


def ring(axis, step):
    count = lax.axis_size(axis)
    return [(i, (i + step) % count) for i in range(count)]


def move(block, axis, step):
    return lax.ppermute(block, axis, ring(axis, step))


def halo(block, dims):
    for dim in dims:
        axis = AXES[dim]
        size = block.shape[dim]
        if lax.axis_size(axis) == 2:
            other = move(block, axis, 1)
            low = lax.slice_in_dim(other, size - 1, size, axis=dim)
            high = lax.slice_in_dim(other, 0, 1, axis=dim)
        else:
            low = lax.slice_in_dim(block, size - 1, size, axis=dim)
            low = move(low, axis, 1)
            high = move(lax.slice_in_dim(block, 0, 1, axis=dim), axis, -1)
        block = jnp.concatenate([low, block, high], axis=dim)
    return block


def cube_root(value):
    return jnp.exp(jnp.log(value) * (1.0 / 3.0))


def split3(value):
    high = value.astype(jnp.bfloat16).astype(jnp.float32)
    rest = value - high
    mid = rest.astype(jnp.bfloat16).astype(jnp.float32)
    return high, mid, rest - mid


def row_index():
    return lax.broadcasted_iota(jnp.int32, (8, 128), 0)


def place(fields, origin):
    row = row_index()
    shift = jnp.where(row == 0, origin[0], jnp.where(row == 1, origin[1], origin[2]))
    spot = jnp.where(row < 3, fields + shift, 0.0)
    return spot, jnp.sum(spot * spot, axis=0, keepdims=True)


def source_rows(spot, square, scale):
    row = row_index()
    value = jnp.where(row == 3, square, jnp.where(row == 4, 1.0, spot)) * scale
    high, mid, low = split3(value)
    return jnp.concatenate([high, mid, high, mid, low, high], axis=0)


def target_rows(spot, square, scale):
    row = row_index()
    value = jnp.where(row == 3, 1.0, jnp.where(row == 4, square, -2.0 * spot)) * scale
    high, mid, low = split3(value)
    return jnp.concatenate([high, high, mid, mid, high, low], axis=0)


def product(left, right):
    return jnp.dot(left, right, preferred_element_type=jnp.float32)


def product_nt(left, right):
    return lax.dot_general(
        left, right, (((1,), (1,)), ((), ())), preferred_element_type=jnp.float32
    )


def product_tn(left, right):
    return lax.dot_general(
        left, right, (((0,), (0,)), ((), ())), preferred_element_type=jnp.float32
    )


def tiled(rows, count):
    return jnp.concatenate([rows] * count, axis=0)


def origin_of(cell, sizes):
    return [c - 0.5 * n for c, n in zip(cell, sizes)]


def cells_of(sizes):
    return [(x, y, z) for x in range(sizes[0]) for y in range(sizes[1]) for z in range(sizes[2])]


def spline(s, root):
    s = jnp.maximum(s, TINY)
    scaled = s * lax.rsqrt(s)
    t = root - scaled
    a = jnp.maximum(t, 0.0)
    b = jnp.maximum(t - scaled, 0.0)
    return a * a * a, b * b * b


def dense_sums(left, dens_ref, root_ref, spans):
    count = left.shape[0]
    near = jnp.zeros((count, 128), jnp.float32)
    far = jnp.zeros((count, 128), jnp.float32)
    for line, lanes, cells in spans:
        s = product(left, dens_ref[line, :, lanes])
        a, b = spline(s, tiled(root_ref[line, :, lanes], count // 8))
        for k in range(cells):
            far = far + a[:, k * 128 : (k + 1) * 128]
            near = near + b[:, k * 128 : (k + 1) * 128]
    return 2.0 * far - near


def row_sums(left, dens_ref, root_ref, spans):
    sums = [
        dense_sums(left[k : k + ROWS], dens_ref, root_ref, spans) for k in range(0, 128, ROWS)
    ]
    return jnp.sum(jnp.concatenate(sums, axis=0).T, axis=0, keepdims=True)


def density_tables(dens_ref, root_ref, line, z, fields, spot, square):
    root = cube_root(fields[3:4])
    part = slice(z * 128, (z + 1) * 128)
    dens_ref[line, :, part] = source_rows(spot, square, root * root).astype(jnp.bfloat16)
    root_ref[line, :, part] = jnp.broadcast_to(root, (8, 128))


def lane_runs(cells, first):
    runs = []
    for z in cells:
        if runs and runs[-1][1] == z:
            runs[-1][1] = z + 1
        else:
            runs.append([z, z + 1])
    return [(slice((a - first) * 128, (b - first) * 128), b - a) for a, b in runs]


def early_kernel(src_ref, len_ref, sum_ref, dens_ref, root_ref, *, sizes, crossing):
    nx, ny, nz = sizes
    cx, cy, cz = nx - 2, ny - 2, nz - 2
    columns = (0, ny - 1) if crossing else tuple(range(1, ny - 1))
    shift = 0 if crossing else 1
    for x, y, z in cells_of((nx, len(columns), cz)):
        fields = src_ref[x, columns[y] - shift, z]
        spot, square = place(fields, origin_of((x, columns[y], z + 1), sizes))
        density_tables(dens_ref, root_ref, x * len(columns) + y, z, fields, spot, square)

    def one_plane(x, carry):
        for y in range(cy):
            for z in range(cz):
                fields = src_ref[x + 1, y + 1 - shift, z]
                where = [x.astype(jnp.float32) + (1.0 - 0.5 * nx)]
                where += [y + 1.0 - 0.5 * ny, z + 1.0 - 0.5 * nz]
                spot, square = place(fields, where)
                inverse = 1.0 / len_ref[x, y, z : z + 1, :]
                left = target_rows(spot, square, inverse * inverse).T.astype(jnp.bfloat16)
                spans = []
                for dx in range(3):
                    for at, source in enumerate(columns):
                        if abs(source - y - 1) <= 1:
                            for lanes, cells in lane_runs(near_of(z + 1, cz), 0):
                                spans.append(((x + dx) * len(columns) + at, lanes, cells))
                total = jnp.zeros((1, 128), jnp.float32)
                if spans:
                    total = row_sums(left, dens_ref, root_ref, spans)
                sum_ref[(x * cy + y) * cz + z] = jnp.broadcast_to(total, (8, 128))
        return carry

    lax.fori_loop(0, cx, one_plane, 0)


def half_up(count):
    return jnp.floor((count + 1.0) * 0.5)


def sort_kernel(src_ref, act_ref, side_ref, *, local):
    row = row_index()
    across = lax.broadcasted_iota(jnp.int32, (128, 128), 0)
    along = lax.broadcasted_iota(jnp.int32, (128, 128), 1)
    earlier = across < along

    def rank(key):
        left = jnp.broadcast_to(key, (8, 128)).T[:, 0:1]
        ahead = (left < key) | (earlier & (left == key))
        return jnp.sum(jnp.where(ahead, 1.0, 0.0), axis=0, keepdims=True)

    for index, cell in enumerate(cells_of(local)):
        fields = src_ref[cell]
        mass = fields[3:4]
        heavy = jnp.where(mass > jnp.sum(mass, axis=1, keepdims=True) * (1.0 / 128.0), 1.0, 0.0)
        light = 128.0 - jnp.sum(heavy, axis=1, keepdims=True)
        base = jnp.zeros((1, 128), jnp.float32)
        size = jnp.broadcast_to(light, (1, 128))
        group = jnp.zeros((1, 128), jnp.float32)
        bits = []
        for dim in range(3):
            place_in = rank(fields[dim : dim + 1] + 2.0 * group + 64.0 * heavy) - base
            first = half_up(size)
            bit = jnp.where(place_in >= first, 1.0, 0.0) * (1.0 - heavy)
            base = base + bit * first
            size = jnp.where(bit > 0.0, size - first, first)
            group = 2.0 * group + bit
            place_in = place_in - bit * first
            bits.append(bit)
        slot = jnp.where(heavy > 0.0, -1.0, 16.0 * group + place_in)
        side = jnp.where(row == 0, bits[0], jnp.where(row == 1, bits[1], bits[2]))
        side = jnp.where(row == 3, heavy, side)
        side = jnp.where(row == 4, slot, side)
        x, y, z = cell
        active = act_ref[x, y, z : z + 1, :].astype(jnp.float32)
        side_ref[index] = jnp.where(row == 5, active, side)


def halves_of(source, count):
    reach = []
    for half in range(2 * count):
        cell = half // 2 + 1
        if source in ((cell - 1, cell) if half % 2 == 0 else (cell, cell + 1)):
            reach.append(half)
    return reach


def near_of(source, count):
    return [c for c in range(count) if abs(c + 1 - source) <= 1]


def runs_of(ranges, counts):
    xs, ys, zs = ranges
    return [
        (((x * counts[1] + y) * counts[2] + zs[0]) * 16, len(zs) * 16) for x in xs for y in ys
    ]


def main_kernel(
    src_ref,
    len_ref,
    side_ref,
    early_ref,
    second_ref,
    rho_ref,
    push_ref,
    heat_ref,
    inner_ref,
    low_ref,
    high_ref,
    dens_ref,
    root_ref,
    flat_ref,
    col_ref,
    size_ref,
    left_ref,
    feat_ref,
    oct_ref,
    rest_ref,
    far_ref,
    close_ref,
    own_ref,
    their_ref,
    sum_ref,
    count_ref,
    *,
    sizes,
):
    nx, ny, nz = sizes
    local = cx, cy, cz = nx - 2, ny - 2, nz - 2
    halves = (2 * cx, 2 * cy, 2 * cz)
    cells = cells_of(local)
    inner = len(cells) * 128
    row = row_index()
    across = lax.broadcasted_iota(jnp.int32, (128, 128), 0)
    along = lax.broadcasted_iota(jnp.int32, (128, 128), 1)
    before = jnp.where(across < along, 1.0, 0.0).astype(jnp.bfloat16)
    slot_of = across.astype(jnp.float32)

    for x, y, z in cells_of(sizes):
        fields = src_ref[x, y, z]
        spot, square = place(fields, origin_of((x, y, z), sizes))
        mass = fields[3:4]
        line = x * ny + y
        part = slice(z * 128, (z + 1) * 128)
        density_tables(dens_ref, root_ref, line, z, fields, spot, square)
        flat_ref[line, :, part] = source_rows(spot, square, 1.0).astype(jnp.bfloat16)
        moving = jnp.sum(fields[4:7] * spot[0:3], axis=0, keepdims=True)
        basis = jnp.where(row < 3, spot, jnp.where(row == 3, 1.0, fields))
        basis = jnp.where(row == 7, moving, basis) * mass
        cols = jnp.concatenate(split3(basis), axis=0).T.astype(jnp.bfloat16)
        col_ref[line, z * 256 : z * 256 + 128, :] = cols
        col_ref[line, z * 256 + 128 : z * 256 + 256, :] = cols

    def first_pass(x, carry):
        for y in range(cy):
            for z in range(cz):
                index = (x * cy + y) * cz + z
                fields = src_ref[x + 1, y + 1, z + 1]
                where = [x.astype(jnp.float32) + (1.0 - 0.5 * nx)]
                where += [y + 1.0 - 0.5 * ny, z + 1.0 - 0.5 * nz]
                spot, square = place(fields, where)
                inverse = 1.0 / len_ref[x, y, z : z + 1, :]
                left = target_rows(spot, square, inverse * inverse).T.astype(jnp.bfloat16)
                spans = []
                for dx in range(3):
                    for source in range(y, y + 3):
                        known = [c + 1 for c in near_of(z + 1, cz)]
                        rest = [c for c in range(z, z + 3) if c not in known]
                        for lanes, cells in lane_runs(rest, 0):
                            spans.append(((x + dx) * ny + source, lanes, cells))
                total = early_ref[index][0:1] + second_ref[index][0:1]
                if spans:
                    total += row_sums(left, dens_ref, root_ref, spans)
                density = kernel_norm * total * (inverse * inverse * inverse)
                length = eta_factor * cube_root(fields[3:4] / density)
                size_ref[index] = jnp.broadcast_to(length, (8, 128))
        return carry

    lax.fori_loop(0, cx, first_pass, 0)

    def cell_runs(cell):
        x, y, z = cell
        return [
            (((2 * x + bx) * halves[1] + 2 * y + by) * halves[2] + 2 * z) * 16
            for bx in range(2)
            for by in range(2)
        ]

    def scatter_rows(ref, cell, value):
        for k, start in enumerate(cell_runs(cell)):
            ref[start : start + 32, :] = value[k * 32 : (k + 1) * 32]

    def gather_rows(value_of, cell):
        return jnp.concatenate([value_of(start) for start in cell_runs(cell)], axis=0)

    def choose(index, fields, length):
        side = side_ref[index]
        reach = jnp.where(side > 0.0, length - fields, fields + length - 1.0)
        wide = jnp.where((row < 3) & (reach > 0.0), 1.0, 0.0)
        wide = jnp.where(row == 3, side, wide)
        wide = jnp.max(wide, axis=0, keepdims=True)
        order = product(jnp.broadcast_to(wide, (8, 128)).astype(jnp.bfloat16), before)[0:1]
        order = jnp.where(wide > 0.0, order, -1.0)
        count_ref[index] = jnp.sum(wide).astype(jnp.int32)
        slot = jnp.where(wide > 0.0, -1.0, side[4:5])
        oct_ref[index] = jnp.where(slot_of == slot, 1.0, 0.0).astype(jnp.bfloat16)
        rest_ref[index] = jnp.broadcast_to(order, (8, 128))

    def picked(index, first, count):
        order = rest_ref[index][0:1] - first
        slots = lax.broadcasted_iota(jnp.int32, (count, 128), 0).astype(jnp.float32)
        return jnp.where(slots == order, 1.0, 0.0)

    def set_rows(index, cell, fields, spot, square, length, weight):
        inverse = 1.0 / length
        choose(index, fields, length)
        count = 16 if weight is None else WIDE
        rest = picked(index, 0.0, count).astype(jnp.bfloat16)
        left = target_rows(spot, square, inverse * inverse).astype(jnp.bfloat16)
        chosen = oct_ref[index]
        scatter_rows(left_ref, cell, product_nt(chosen, left).astype(jnp.bfloat16))
        part = slice(inner + index * WIDE, inner + index * WIDE + count)
        left_ref[part, :] = product_nt(rest, left).astype(jnp.bfloat16)
        if weight is not None:
            feat = jnp.concatenate(split3(weight), axis=0).astype(jnp.bfloat16)
            scatter_rows(feat_ref, cell, product_nt(chosen, feat).astype(jnp.bfloat16))
            feat_ref[part, :] = product_nt(rest, feat).astype(jnp.bfloat16)

    def source_runs(x, y, z, count):
        ranges = [halves_of(s, n) for s, n in zip((x, y, z), local)]
        runs = runs_of(ranges, halves)
        ranges = [near_of(s, n) for s, n in zip((x, y, z), local)]
        for start, size in runs_of(ranges, local):
            for first in range(start // 16, (start + size) // 16):
                runs.append((inner + first * WIDE, count))
        return runs

    def rows_of(ref, runs):
        return jnp.concatenate([ref[start : start + size, :] for start, size in runs], axis=0)

    def add_rows(ref, runs, value):
        at = 0
        for start, size in runs:
            ref[start : start + size, :] += value[at : at + size]
            at += size

    def unsorted_column(index, octant, rest):
        total = jnp.sum(octant, axis=1, keepdims=True) * oct_ref[index].astype(jnp.float32)
        total = jnp.sum(total, axis=0, keepdims=True)
        rest = jnp.sum(rest, axis=1, keepdims=True) * picked(index, 0.0, 16)
        return total + jnp.sum(rest, axis=0, keepdims=True)

    def extras(visit, first):
        def one_cell(index, carry):
            def one_chunk(chunk, carry):
                x = index // (cy * cz)
                y = index // cz % cy
                z = index % cz
                fields = src_ref[x + 1, y + 1, z + 1]
                where = [v.astype(jnp.float32) + (1.0 - 0.5 * n) for v, n in zip((x, y, z), sizes)]
                spot, square = place(fields, where)
                inverse = 1.0 / size_ref[index][0:1]
                rest = picked(index, chunk.astype(jnp.float32) * 16.0, 16)
                left = target_rows(spot, square, inverse * inverse).astype(jnp.bfloat16)
                left = product_nt(rest.astype(jnp.bfloat16), left).astype(jnp.bfloat16)
                visit(index, (x, y, z), fields, spot, rest, left)
                return carry

            return lax.fori_loop(first, (count_ref[index] + 15) // 16, one_chunk, carry)

        lax.fori_loop(0, cx * cy * cz, one_cell, 0)

    def weight_of(fields, spot, strength):
        return jnp.where(row < 3, spot, jnp.where(row == 3, 1.0, 0.0)) * (fields[3:4] * strength)

    def extra_density(index, cell, fields, spot, rest, left):
        x, y, z = cell
        lanes = pl.ds(pl.multiple_of(z * 128, 128), 384)
        spans = [((x + dx) * ny + y + dy, lanes, 3) for dx in range(3) for dy in range(3)]
        extra = dense_sums(left, dens_ref, root_ref, spans)
        extra = jnp.sum(extra, axis=1, keepdims=True) * rest
        sum_ref[index, 0:8, :] += jnp.sum(extra, axis=0, keepdims=True)

    def unsort(value, rest):
        pieces = split3(value)
        rest = rest.astype(jnp.bfloat16)
        total = product_tn(pieces[0].astype(jnp.bfloat16), rest)
        total += product_tn(pieces[1].astype(jnp.bfloat16), rest)
        return total + product_tn(pieces[2].astype(jnp.bfloat16), rest)

    def extra_force(index, cell, fields, spot, rest, left):
        x, y, z = cell
        feat = jnp.concatenate(split3(weight_of(fields, spot, size_ref[index][1:2])), axis=0)
        feat = product_nt(rest.astype(jnp.bfloat16), feat.astype(jnp.bfloat16))
        feat = feat.astype(jnp.bfloat16)
        total = jnp.zeros((16, 24), jnp.float32)
        for dx in range(3):
            for dy in range(3):
                line = (x + dx) * ny + y + dy
                lanes = pl.ds(pl.multiple_of(z * 128, 128), 384)
                high, low = profile(product(left, flat_ref[line, :, lanes]))
                for dz in range(3):
                    cols = col_ref[line, pl.ds(pl.multiple_of((z + dz) * 256, 256), 256), :]
                    part = slice(dz * 128, (dz + 1) * 128)
                    pair = jnp.concatenate([high[:, part], low[:, part]], axis=1)
                    total += product(pair, cols)
                their_ref[line, :, lanes] += product_tn(feat, high) + product_tn(feat, low)
        sum_ref[index] += unsort(total, rest)

    placed = []
    for index, cell in enumerate(cells):
        fields = src_ref[cell[0] + 1, cell[1] + 1, cell[2] + 1]
        origin = origin_of([c + 1 for c in cell], sizes)
        placed.append((fields, origin))
        spot, square = place(fields, origin)
        set_rows(index, cell, fields, spot, square, size_ref[index][0:1], None)

    far_ref[...] = jnp.zeros_like(far_ref)
    close_ref[...] = jnp.zeros_like(close_ref)
    for x, y, z in cells_of(sizes):
        runs = source_runs(x, y, z, 16)
        line = x * ny + y
        part = slice(z * 128, (z + 1) * 128)
        left = rows_of(left_ref, runs)
        s = product(left, dens_ref[line, :, part])
        a, b = spline(s, tiled(root_ref[line, :, part], left.shape[0] // 8))
        add_rows(far_ref, runs, a)
        add_rows(close_ref, runs, b)

    for index, cell in enumerate(cells):
        part = slice(inner + index * WIDE, inner + index * WIDE + 16)
        octant = gather_rows(
            lambda start: 2.0 * far_ref[start : start + 32, :] - close_ref[start : start + 32, :],
            cell,
        )
        total = unsorted_column(index, octant, 2.0 * far_ref[part, :] - close_ref[part, :])
        sum_ref[index, 0:8, :] = jnp.broadcast_to(total, (8, 128))
    extras(extra_density, 1)
    for index, cell in enumerate(cells):
        x, y, z = cell
        fields, origin = placed[index]
        spot, square = place(fields, origin)
        inverse = 1.0 / size_ref[index][0:1]
        density = kernel_norm * sum_ref[index, 0:1, :] * (inverse * inverse * inverse)
        rho_ref[x, y, z : z + 1, :] = density
        length = eta_factor * cube_root(fields[3:4] / density)
        _, strength = smooth(fields, density)
        size_ref[index] = jnp.where(row == 0, length, strength)
        set_rows(index, cell, fields, spot, square, length, weight_of(fields, spot, strength))

    own_ref[...] = jnp.zeros_like(own_ref)

    def slopes(x, y, z):
        runs = source_runs(x, y, z, WIDE)
        line = x * ny + y
        part = slice(z * 128, (z + 1) * 128)
        high, low = profile(product(rows_of(left_ref, runs), flat_ref[line, :, part]))
        return line, z, runs, high, low

    def sums(line, z, runs, high, low):
        part = slice(z * 128, (z + 1) * 128)
        cols = col_ref[line, z * 256 : (z + 1) * 256, :]
        add_rows(own_ref, runs, product(jnp.concatenate([high, low], axis=1), cols))
        feat = rows_of(feat_ref, runs)
        their_ref[line, :, part] = product_tn(feat, high) + product_tn(feat, low)

    waiting = None
    for source in cells_of(sizes):
        ready = slopes(*source)
        if waiting is not None:
            sums(*waiting)
        waiting = ready
    sums(*waiting)

    for index, cell in enumerate(cells):
        octant = gather_rows(lambda start: own_ref[start : start + 32, :], cell)
        part = slice(inner + index * WIDE, inner + index * WIDE + WIDE)
        own = unsort(octant, oct_ref[index]) + unsort(own_ref[part, :], picked(index, 0.0, WIDE))
        sum_ref[index] = own
    extras(extra_force, WIDE // 16)
    for index, cell in enumerate(cells):
        x, y, z = cell
        fields, origin = placed[index]
        spot, square = place(fields, origin)
        own = sum_ref[index]
        own = (own[0:8] + own[8:16] + own[16:24]) * size_ref[index][1:2]
        active = side_ref[index, 5:6, :]
        spot = spot[0:3]
        push = spot * own[3:4] - own[0:3]
        heat = fields[4:7] * push - spot * own[4:7]
        heat = jnp.sum(heat, axis=0, keepdims=True) + own[7:8]
        push_ref[x, y, z] = jnp.concatenate([push, active], axis=0)
        heat_ref[x, y, z : z + 1, :] = active * heat

    for x, y, z in cells_of(sizes):
        spot, square = place(src_ref[x, y, z], origin_of((x, y, z), sizes))
        their = their_ref[x * ny + y, :, z * 128 : (z + 1) * 128]
        their = their[0:8] + their[8:16] + their[16:24]
        their = (spot * their[3:4] - their)[0:4]
        if z == 0:
            low_ref[x, y, 0] = their
        elif z == nz - 1:
            high_ref[x, y, 0] = their
        else:
            inner_ref[x, y, z - 1] = their


def profile(s):
    s = jnp.maximum(s, TINY)
    rs = lax.rsqrt(s)
    q = s * rs
    t = 1.0 - q
    a = jnp.maximum(t, 0.0)
    b = jnp.maximum(t - q, 0.0)
    g = jnp.minimum(a, q) * (a + b) * rs
    high = g.astype(jnp.bfloat16)
    return high, (g - high.astype(jnp.float32)).astype(jnp.bfloat16)


def smooth(fields, density):
    inverse = 1.0 / (eta_factor * cube_root(fields[3:4] / density))
    inv2 = inverse * inverse
    press = (gamma_index - 1.0) * fields[7:8] / density
    return inv2, press * (-6.0 * kernel_norm) * inv2 * inv2 * inverse


def take(block, dim, start, stop):
    return lax.slice_in_dim(block, start, stop, axis=dim)


def fold(block, low, high):
    for dim in (2, 1, 0):
        axis = AXES[dim]
        if dim < 2:
            last = block.shape[dim] - 1
            low, high = take(block, dim, 0, 1), take(block, dim, last, last + 1)
            block = take(block, dim, 1, last)
        if lax.axis_size(axis) == 2:
            both = lax.ppermute(jnp.concatenate([high, low], axis=dim), axis, ring(axis, 1))
            to_first, to_last = take(both, dim, 0, 1), take(both, dim, 1, 2)
        else:
            to_last = lax.ppermute(low, axis, ring(axis, -1))
            to_first = lax.ppermute(high, axis, ring(axis, 1))
        count = block.shape[dim]
        if count == 1:
            block = block + to_first + to_last
        else:
            block = jnp.concatenate(
                [
                    take(block, dim, 0, 1) + to_first,
                    take(block, dim, 1, count - 1),
                    take(block, dim, count - 1, count) + to_last,
                ],
                axis=dim,
            )
    return block


def body(offsets, masses, smoothing, velocity, energy, active):
    local = masses.shape[:3]
    sizes = tuple(n + 2 for n in local)
    nx, ny, nz = sizes
    f32 = jnp.float32
    bf16 = jnp.bfloat16
    ncell = local[0] * local[1] * local[2]
    static = jnp.stack(
        [offsets[0], offsets[1], offsets[2], masses, velocity[0], velocity[1], velocity[2], energy],
        axis=3,
    )
    side = pl.pallas_call(
        functools.partial(sort_kernel, local=local),
        out_shape=jax.ShapeDtypeStruct((ncell, 8, 128), f32),
        compiler_params=pltpu.CompilerParams(vmem_limit_bytes=VMEM_LIMIT),
        name="sort",
    )(static, active)
    wide = halo(static, (0,))

    def begin(block, crossing):
        lines = nx * (2 if crossing else local[1])
        return pl.pallas_call(
            functools.partial(early_kernel, sizes=sizes, crossing=crossing),
            out_shape=jax.ShapeDtypeStruct((ncell, 8, 128), f32),
            scratch_shapes=[
                pltpu.VMEM((lines, 48, local[2] * 128), bf16),
                pltpu.VMEM((lines, 8, local[2] * 128), f32),
            ],
            compiler_params=pltpu.CompilerParams(vmem_limit_bytes=VMEM_LIMIT),
        )(block, smoothing)

    early = begin(wide, False)
    tall = halo(wide, (1,))
    second = begin(tall, True)
    padded = halo(tall, (2,))
    lines = nx * ny
    rows = ncell * (128 + WIDE)
    density, push, heat, spread, low, high = pl.pallas_call(
        functools.partial(main_kernel, sizes=sizes),
        out_shape=(
            jax.ShapeDtypeStruct(masses.shape, f32),
            jax.ShapeDtypeStruct(local + (4, 128), f32),
            jax.ShapeDtypeStruct(masses.shape, f32),
            jax.ShapeDtypeStruct((nx, ny, local[2], 4, 128), f32),
            jax.ShapeDtypeStruct((nx, ny, 1, 4, 128), f32),
            jax.ShapeDtypeStruct((nx, ny, 1, 4, 128), f32),
        ),
        scratch_shapes=[
            pltpu.VMEM((lines, 48, nz * 128), bf16),
            pltpu.VMEM((lines, 8, nz * 128), f32),
            pltpu.VMEM((lines, 48, nz * 128), bf16),
            pltpu.VMEM((lines, nz * 256, 24), bf16),
            pltpu.VMEM((ncell, 8, 128), f32),
            pltpu.VMEM((rows, 48), bf16),
            pltpu.VMEM((rows, 24), bf16),
            pltpu.VMEM((ncell, 128, 128), bf16),
            pltpu.VMEM((ncell, 8, 128), f32),
            pltpu.VMEM((rows, 128), f32),
            pltpu.VMEM((rows, 128), f32),
            pltpu.VMEM((rows, 24), f32),
            pltpu.VMEM((lines, 24, nz * 128), f32),
            pltpu.VMEM((ncell, 24, 128), f32),
            pltpu.SMEM((ncell,), jnp.int32),
        ],
        compiler_params=pltpu.CompilerParams(vmem_limit_bytes=VMEM_LIMIT),
        name="main",
    )(padded, smoothing, side, early, second)
    total = -(push[..., 0:3, :] + fold(spread, low, high)[..., 0:3, :]) * push[..., 3:4, :]
    return (density, jnp.moveaxis(total, 3, 0), heat)


def solution(mesh):
    vector = P(None, "gx", "gy", "gz", None)
    scalar = P("gx", "gy", "gz", None)
    return jax.shard_map(
        body,
        mesh=mesh,
        in_specs=(vector, scalar, scalar, vector, scalar, scalar),
        out_specs=(scalar, vector, scalar),
        check_vma=False,
    )
```

```python
import functools

import jax
import jax.numpy as jnp
from jax import lax
from jax.experimental import pallas as pl
from jax.experimental.pallas import tpu as pltpu
from jax.sharding import PartitionSpec as P


kernel_norm = 2.5464790894703255
eta_factor = 2.3
gamma_index = 5.0 / 3.0

ROWS = 32
TINY = 1e-12
WIDE = 32
VMEM_LIMIT = 24 * 1024 * 1024
AXES = ("gx", "gy", "gz")


def ring(axis, step):
    count = lax.axis_size(axis)
    return [(i, (i + step) % count) for i in range(count)]


def move(block, axis, step):
    return lax.ppermute(block, axis, ring(axis, step))


def halo(block, dims):
    for dim in dims:
        axis = AXES[dim]
        size = block.shape[dim]
        if lax.axis_size(axis) == 2:
            other = move(block, axis, 1)
            low = lax.slice_in_dim(other, size - 1, size, axis=dim)
            high = lax.slice_in_dim(other, 0, 1, axis=dim)
        else:
            low = lax.slice_in_dim(block, size - 1, size, axis=dim)
            low = move(low, axis, 1)
            high = move(lax.slice_in_dim(block, 0, 1, axis=dim), axis, -1)
        block = jnp.concatenate([low, block, high], axis=dim)
    return block


def cube_root(value):
    return jnp.exp(jnp.log(value) * (1.0 / 3.0))


def split3(value):
    high = value.astype(jnp.bfloat16).astype(jnp.float32)
    rest = value - high
    mid = rest.astype(jnp.bfloat16).astype(jnp.float32)
    return high, mid, rest - mid


def row_index():
    return lax.broadcasted_iota(jnp.int32, (8, 128), 0)


def place(fields, origin):
    row = row_index()
    shift = jnp.where(row == 0, origin[0], jnp.where(row == 1, origin[1], origin[2]))
    spot = jnp.where(row < 3, fields + shift, 0.0)
    return spot, jnp.sum(spot * spot, axis=0, keepdims=True)


def source_rows(spot, square, scale):
    row = row_index()
    value = jnp.where(row == 3, square, jnp.where(row == 4, 1.0, spot)) * scale
    high, mid, low = split3(value)
    return jnp.concatenate([high, mid, high, mid, low, high], axis=0)


def target_rows(spot, square, scale):
    row = row_index()
    value = jnp.where(row == 3, 1.0, jnp.where(row == 4, square, -2.0 * spot)) * scale
    high, mid, low = split3(value)
    return jnp.concatenate([high, high, mid, mid, high, low], axis=0)


def product(left, right):
    return jnp.dot(left, right, preferred_element_type=jnp.float32)


def product_nt(left, right):
    return lax.dot_general(
        left, right, (((1,), (1,)), ((), ())), preferred_element_type=jnp.float32
    )


def product_tn(left, right):
    return lax.dot_general(
        left, right, (((0,), (0,)), ((), ())), preferred_element_type=jnp.float32
    )


def tiled(rows, count):
    return jnp.concatenate([rows] * count, axis=0)


def origin_of(cell, sizes):
    return [c - 0.5 * n for c, n in zip(cell, sizes)]


def cells_of(sizes):
    return [(x, y, z) for x in range(sizes[0]) for y in range(sizes[1]) for z in range(sizes[2])]


def spline(s, root):
    s = jnp.maximum(s, TINY)
    scaled = s * lax.rsqrt(s)
    t = root - scaled
    a = jnp.maximum(t, 0.0)
    b = jnp.maximum(t - scaled, 0.0)
    return a * a * a, b * b * b


def dense_sums(left, dens_ref, root_ref, spans):
    count = left.shape[0]
    near = jnp.zeros((count, 128), jnp.float32)
    far = jnp.zeros((count, 128), jnp.float32)
    for line, lanes, cells in spans:
        s = product(left, dens_ref[line, :, lanes])
        a, b = spline(s, tiled(root_ref[line, :, lanes], count // 8))
        for k in range(cells):
            far = far + a[:, k * 128 : (k + 1) * 128]
            near = near + b[:, k * 128 : (k + 1) * 128]
    return 2.0 * far - near


def row_sums(left, dens_ref, root_ref, spans):
    sums = [
        dense_sums(left[k : k + ROWS], dens_ref, root_ref, spans) for k in range(0, 128, ROWS)
    ]
    return jnp.sum(jnp.concatenate(sums, axis=0).T, axis=0, keepdims=True)


def density_tables(dens_ref, root_ref, line, z, fields, spot, square):
    root = cube_root(fields[3:4])
    part = slice(z * 128, (z + 1) * 128)
    dens_ref[line, :, part] = source_rows(spot, square, root * root).astype(jnp.bfloat16)
    root_ref[line, :, part] = jnp.broadcast_to(root, (8, 128))


def lane_runs(cells, first):
    runs = []
    for z in cells:
        if runs and runs[-1][1] == z:
            runs[-1][1] = z + 1
        else:
            runs.append([z, z + 1])
    return [(slice((a - first) * 128, (b - first) * 128), b - a) for a, b in runs]


def early_kernel(src_ref, len_ref, sum_ref, dens_ref, root_ref, *, sizes, crossing):
    nx, ny, nz = sizes
    cx, cy, cz = nx - 2, ny - 2, nz - 2
    columns = (0, ny - 1) if crossing else tuple(range(1, ny - 1))
    shift = 0 if crossing else 1
    for x, y, z in cells_of((nx, len(columns), cz)):
        fields = src_ref[x, columns[y] - shift, z]
        spot, square = place(fields, origin_of((x, columns[y], z + 1), sizes))
        density_tables(dens_ref, root_ref, x * len(columns) + y, z, fields, spot, square)

    def one_plane(x, carry):
        for y in range(cy):
            for z in range(cz):
                fields = src_ref[x + 1, y + 1 - shift, z]
                where = [x.astype(jnp.float32) + (1.0 - 0.5 * nx)]
                where += [y + 1.0 - 0.5 * ny, z + 1.0 - 0.5 * nz]
                spot, square = place(fields, where)
                inverse = 1.0 / len_ref[x, y, z : z + 1, :]
                left = target_rows(spot, square, inverse * inverse).T.astype(jnp.bfloat16)
                spans = []
                for dx in range(3):
                    for at, source in enumerate(columns):
                        if abs(source - y - 1) <= 1:
                            for lanes, cells in lane_runs(near_of(z + 1, cz), 0):
                                spans.append(((x + dx) * len(columns) + at, lanes, cells))
                total = jnp.zeros((1, 128), jnp.float32)
                if spans:
                    total = row_sums(left, dens_ref, root_ref, spans)
                sum_ref[(x * cy + y) * cz + z] = jnp.broadcast_to(total, (8, 128))
        return carry

    lax.fori_loop(0, cx, one_plane, 0)


def half_up(count):
    return jnp.floor((count + 1.0) * 0.5)


def sort_kernel(src_ref, act_ref, side_ref, *, local):
    row = row_index()
    across = lax.broadcasted_iota(jnp.int32, (128, 128), 0)
    along = lax.broadcasted_iota(jnp.int32, (128, 128), 1)
    earlier = across < along

    def rank(key):
        left = jnp.broadcast_to(key, (8, 128)).T[:, 0:1]
        ahead = (left < key) | (earlier & (left == key))
        return jnp.sum(jnp.where(ahead, 1.0, 0.0), axis=0, keepdims=True)

    for index, cell in enumerate(cells_of(local)):
        fields = src_ref[cell]
        mass = fields[3:4]
        heavy = jnp.where(mass > jnp.sum(mass, axis=1, keepdims=True) * (1.0 / 128.0), 1.0, 0.0)
        light = 128.0 - jnp.sum(heavy, axis=1, keepdims=True)
        base = jnp.zeros((1, 128), jnp.float32)
        size = jnp.broadcast_to(light, (1, 128))
        group = jnp.zeros((1, 128), jnp.float32)
        bits = []
        for dim in range(3):
            place_in = rank(fields[dim : dim + 1] + 2.0 * group + 64.0 * heavy) - base
            first = half_up(size)
            bit = jnp.where(place_in >= first, 1.0, 0.0) * (1.0 - heavy)
            base = base + bit * first
            size = jnp.where(bit > 0.0, size - first, first)
            group = 2.0 * group + bit
            place_in = place_in - bit * first
            bits.append(bit)
        slot = jnp.where(heavy > 0.0, -1.0, 16.0 * group + place_in)
        side = jnp.where(row == 0, bits[0], jnp.where(row == 1, bits[1], bits[2]))
        side = jnp.where(row == 3, heavy, side)
        side = jnp.where(row == 4, slot, side)
        x, y, z = cell
        active = act_ref[x, y, z : z + 1, :].astype(jnp.float32)
        side_ref[index] = jnp.where(row == 5, active, side)


def halves_of(source, count):
    reach = []
    for half in range(2 * count):
        cell = half // 2 + 1
        if source in ((cell - 1, cell) if half % 2 == 0 else (cell, cell + 1)):
            reach.append(half)
    return reach


def near_of(source, count):
    return [c for c in range(count) if abs(c + 1 - source) <= 1]


def runs_of(ranges, counts):
    xs, ys, zs = ranges
    return [
        (((x * counts[1] + y) * counts[2] + zs[0]) * 16, len(zs) * 16) for x in xs for y in ys
    ]


def cell_runs(cell, halves):
    x, y, z = cell
    return [
        (((2 * x + bx) * halves[1] + 2 * y + by) * halves[2] + 2 * z) * 16
        for bx in range(2)
        for by in range(2)
    ]


def scatter_rows(ref, cell, halves, value):
    for k, start in enumerate(cell_runs(cell, halves)):
        ref[start : start + 32, :] = value[k * 32 : (k + 1) * 32]


def gather_rows(value_of, cell, halves):
    return jnp.concatenate([value_of(start) for start in cell_runs(cell, halves)], axis=0)


def source_runs(source, local, count):
    inner = 128 * local[0] * local[1] * local[2]
    ranges = [halves_of(s, n) for s, n in zip(source, local)]
    runs = runs_of(ranges, [2 * n for n in local])
    ranges = [near_of(s, n) for s, n in zip(source, local)]
    for start, size in runs_of(ranges, local):
        for first in range(start // 16, (start + size) // 16):
            runs.append((inner + first * WIDE, count))
    return runs


def rows_of(ref, runs):
    return jnp.concatenate([ref[start : start + size, :] for start, size in runs], axis=0)


def add_rows(ref, runs, value):
    at = 0
    for start, size in runs:
        ref[start : start + size, :] += value[at : at + size]
        at += size


def picked(rest_ref, index, first, count):
    order = rest_ref[index][0:1] - first
    slots = lax.broadcasted_iota(jnp.int32, (count, 128), 0).astype(jnp.float32)
    return jnp.where(slots == order, 1.0, 0.0)


def unsort(value, rest):
    pieces = split3(value)
    rest = rest.astype(jnp.bfloat16)
    total = product_tn(pieces[0].astype(jnp.bfloat16), rest)
    total += product_tn(pieces[1].astype(jnp.bfloat16), rest)
    return total + product_tn(pieces[2].astype(jnp.bfloat16), rest)


def force_columns(fields, spot):
    row = row_index()
    moving = jnp.sum(fields[4:7] * spot[0:3], axis=0, keepdims=True)
    basis = jnp.where(row < 3, spot, jnp.where(row == 3, 1.0, fields))
    basis = jnp.where(row == 7, moving, basis) * fields[3:4]
    return jnp.concatenate(split3(basis), axis=0).T.astype(jnp.bfloat16)


def force_sums(sources, left_ref, feat_ref, own_ref, flat_of, cols_of, put, local):
    def sums(source, runs, high, low):
        add_rows(own_ref, runs, product(jnp.concatenate([high, low], axis=1), cols_of(source)))
        feat = rows_of(feat_ref, runs)
        put(source, product_tn(feat, high) + product_tn(feat, low))

    waiting = None
    for source in sources:
        runs = source_runs(source, local, WIDE)
        high, low = profile(product(rows_of(left_ref, runs), flat_of(source)))
        if waiting is not None:
            sums(*waiting)
        waiting = (source, runs, high, low)
    sums(*waiting)


def is_local(cell, local):
    return all(0 < c <= n for c, n in zip(cell, local))


def edge_kernel(
    src_ref, left_ref, feat_ref, own_ref, low_ref, high_ref, flat_ref, col_ref, *, sizes, dim
):
    local = tuple(n - 2 for n in sizes)
    ends = (0, sizes[dim] - 1)
    numbers = {}
    for cell in cells_of(sizes):
        if cell[dim] in ends and all(0 < cell[k] <= local[k] for k in range(dim + 1, 3)):
            if dim == 1 or is_local(cell[1:], local[1:]):
                numbers[cell] = len(numbers)
    for cell, index in numbers.items():
        fields = src_ref[cell]
        spot, square = place(fields, origin_of(cell, sizes))
        flat_ref[index] = source_rows(spot, square, 1.0).astype(jnp.bfloat16)
        cols = force_columns(fields, spot)
        col_ref[index, 0:128, :] = cols
        col_ref[index, 128:256, :] = cols
    own_ref[...] = jnp.zeros_like(own_ref)

    def put(source, value):
        spot, _ = place(src_ref[source], origin_of(source, sizes))
        their = value[0:8] + value[8:16] + value[16:24]
        at = [c if k < dim else c - 1 for k, c in enumerate(source)]
        at[dim] = 0
        ref = low_ref if source[dim] == 0 else high_ref
        ref[tuple(at)] = (spot * their[3:4] - their)[0:4]

    force_sums(
        list(numbers),
        left_ref,
        feat_ref,
        own_ref,
        lambda source: flat_ref[numbers[source]],
        lambda source: col_ref[numbers[source]],
        put,
        local,
    )


def rest_kernel(
    src_ref,
    side_ref,
    size_ref,
    left_ref,
    feat_ref,
    oct_ref,
    rest_ref,
    part_ref,
    sum_ref,
    wide_ref,
    tall_ref,
    push_ref,
    heat_ref,
    flat_ref,
    col_ref,
    own_ref,
    their_ref,
    *,
    sizes,
):
    local = tuple(n - 2 for n in sizes)
    halves = [2 * n for n in local]
    cells = cells_of(local)
    inner = 128 * len(cells)
    numbers = {tuple(c + 1 for c in cell): k for k, cell in enumerate(cells)}
    places = []
    for index, cell in enumerate(cells):
        fields = src_ref[cell]
        spot, square = place(fields, origin_of([c + 1 for c in cell], sizes))
        flat_ref[index] = source_rows(spot, square, 1.0).astype(jnp.bfloat16)
        cols = force_columns(fields, spot)
        col_ref[index, 0:128, :] = cols
        col_ref[index, 128:256, :] = cols
        places.append((fields, spot[0:3]))
    own_ref[...] = part_ref[...] + wide_ref[...] + tall_ref[...]

    def put(source, value):
        their_ref[numbers[source]] = value

    force_sums(
        list(numbers),
        left_ref,
        feat_ref,
        own_ref,
        lambda source: flat_ref[numbers[source]],
        lambda source: col_ref[numbers[source]],
        put,
        local,
    )
    for index, cell in enumerate(cells):
        fields, spot = places[index]
        octant = gather_rows(lambda start: own_ref[start : start + 32, :], cell, halves)
        part = slice(inner + index * WIDE, inner + index * WIDE + WIDE)
        own = unsort(octant, oct_ref[index]) + sum_ref[index]
        own += unsort(own_ref[part, :], picked(rest_ref, index, 0.0, WIDE))
        own = (own[0:8] + own[8:16] + own[16:24]) * size_ref[index][1:2]
        their = their_ref[index]
        their = their[0:8] + their[8:16] + their[16:24]
        active = side_ref[index, 5:6, :]
        push = spot * own[3:4] - own[0:3]
        heat = fields[4:7] * push - spot * own[4:7]
        heat = jnp.sum(heat, axis=0, keepdims=True) + own[7:8]
        push = push + spot * their[3:4] - their[0:3]
        push_ref[cell] = jnp.concatenate([push, active], axis=0)
        heat_ref[cell[0], cell[1], cell[2] : cell[2] + 1, :] = active * heat


def main_kernel(
    src_ref,
    len_ref,
    side_ref,
    early_ref,
    second_ref,
    rho_ref,
    inner_ref,
    low_ref,
    high_ref,
    size_ref,
    left_ref,
    feat_ref,
    oct_ref,
    rest_ref,
    own_ref,
    sum_ref,
    dens_ref,
    root_ref,
    flat_ref,
    col_ref,
    far_ref,
    close_ref,
    their_ref,
    count_ref,
    *,
    sizes,
):
    nx, ny, nz = sizes
    local = cx, cy, cz = nx - 2, ny - 2, nz - 2
    halves = (2 * cx, 2 * cy, 2 * cz)
    cells = cells_of(local)
    inner = len(cells) * 128
    row = row_index()
    across = lax.broadcasted_iota(jnp.int32, (128, 128), 0)
    along = lax.broadcasted_iota(jnp.int32, (128, 128), 1)
    before = jnp.where(across < along, 1.0, 0.0).astype(jnp.bfloat16)
    slot_of = across.astype(jnp.float32)

    for x, y, z in cells_of(sizes):
        fields = src_ref[x, y, z]
        spot, square = place(fields, origin_of((x, y, z), sizes))
        line = x * ny + y
        part = slice(z * 128, (z + 1) * 128)
        density_tables(dens_ref, root_ref, line, z, fields, spot, square)
        flat_ref[line, :, part] = source_rows(spot, square, 1.0).astype(jnp.bfloat16)
        cols = force_columns(fields, spot)
        col_ref[line, z * 256 : z * 256 + 128, :] = cols
        col_ref[line, z * 256 + 128 : z * 256 + 256, :] = cols

    def first_pass(x, carry):
        for y in range(cy):
            for z in range(cz):
                index = (x * cy + y) * cz + z
                fields = src_ref[x + 1, y + 1, z + 1]
                where = [x.astype(jnp.float32) + (1.0 - 0.5 * nx)]
                where += [y + 1.0 - 0.5 * ny, z + 1.0 - 0.5 * nz]
                spot, square = place(fields, where)
                inverse = 1.0 / len_ref[x, y, z : z + 1, :]
                left = target_rows(spot, square, inverse * inverse).T.astype(jnp.bfloat16)
                spans = []
                for dx in range(3):
                    for source in range(y, y + 3):
                        known = [c + 1 for c in near_of(z + 1, cz)]
                        rest = [c for c in range(z, z + 3) if c not in known]
                        for lanes, cells in lane_runs(rest, 0):
                            spans.append(((x + dx) * ny + source, lanes, cells))
                total = early_ref[index][0:1] + second_ref[index][0:1]
                if spans:
                    total += row_sums(left, dens_ref, root_ref, spans)
                density = kernel_norm * total * (inverse * inverse * inverse)
                length = eta_factor * cube_root(fields[3:4] / density)
                size_ref[index] = jnp.broadcast_to(length, (8, 128))
        return carry

    lax.fori_loop(0, cx, first_pass, 0)

    def choose(index, fields, length):
        side = side_ref[index]
        reach = jnp.where(side > 0.0, length - fields, fields + length - 1.0)
        wide = jnp.where((row < 3) & (reach > 0.0), 1.0, 0.0)
        wide = jnp.where(row == 3, side, wide)
        wide = jnp.max(wide, axis=0, keepdims=True)
        order = product(jnp.broadcast_to(wide, (8, 128)).astype(jnp.bfloat16), before)[0:1]
        order = jnp.where(wide > 0.0, order, -1.0)
        count_ref[index] = jnp.sum(wide).astype(jnp.int32)
        slot = jnp.where(wide > 0.0, -1.0, side[4:5])
        oct_ref[index] = jnp.where(slot_of == slot, 1.0, 0.0).astype(jnp.bfloat16)
        rest_ref[index] = jnp.broadcast_to(order, (8, 128))

    def set_rows(index, cell, fields, spot, square, length, weight):
        inverse = 1.0 / length
        choose(index, fields, length)
        count = 16 if weight is None else WIDE
        rest = picked(rest_ref, index, 0.0, count).astype(jnp.bfloat16)
        left = target_rows(spot, square, inverse * inverse).astype(jnp.bfloat16)
        chosen = oct_ref[index]
        scatter_rows(left_ref, cell, halves, product_nt(chosen, left).astype(jnp.bfloat16))
        part = slice(inner + index * WIDE, inner + index * WIDE + count)
        left_ref[part, :] = product_nt(rest, left).astype(jnp.bfloat16)
        if weight is not None:
            feat = jnp.concatenate(split3(weight), axis=0).astype(jnp.bfloat16)
            scatter_rows(feat_ref, cell, halves, product_nt(chosen, feat).astype(jnp.bfloat16))
            feat_ref[part, :] = product_nt(rest, feat).astype(jnp.bfloat16)

    def unsorted_column(index, octant, rest):
        total = jnp.sum(octant, axis=1, keepdims=True) * oct_ref[index].astype(jnp.float32)
        total = jnp.sum(total, axis=0, keepdims=True)
        rest = jnp.sum(rest, axis=1, keepdims=True) * picked(rest_ref, index, 0.0, 16)
        return total + jnp.sum(rest, axis=0, keepdims=True)

    def extras(visit, first):
        def one_cell(index, carry):
            def one_chunk(chunk, carry):
                x = index // (cy * cz)
                y = index // cz % cy
                z = index % cz
                fields = src_ref[x + 1, y + 1, z + 1]
                where = [v.astype(jnp.float32) + (1.0 - 0.5 * n) for v, n in zip((x, y, z), sizes)]
                spot, square = place(fields, where)
                inverse = 1.0 / size_ref[index][0:1]
                rest = picked(rest_ref, index, chunk.astype(jnp.float32) * 16.0, 16)
                left = target_rows(spot, square, inverse * inverse).astype(jnp.bfloat16)
                left = product_nt(rest.astype(jnp.bfloat16), left).astype(jnp.bfloat16)
                visit(index, (x, y, z), fields, spot, rest, left)
                return carry

            return lax.fori_loop(first, (count_ref[index] + 15) // 16, one_chunk, carry)

        lax.fori_loop(0, cx * cy * cz, one_cell, 0)

    def weight_of(fields, spot, strength):
        return jnp.where(row < 3, spot, jnp.where(row == 3, 1.0, 0.0)) * (fields[3:4] * strength)

    def extra_density(index, cell, fields, spot, rest, left):
        x, y, z = cell
        lanes = pl.ds(pl.multiple_of(z * 128, 128), 384)
        spans = [((x + dx) * ny + y + dy, lanes, 3) for dx in range(3) for dy in range(3)]
        extra = dense_sums(left, dens_ref, root_ref, spans)
        extra = jnp.sum(extra, axis=1, keepdims=True) * rest
        sum_ref[index, 0:8, :] += jnp.sum(extra, axis=0, keepdims=True)

    def extra_force(index, cell, fields, spot, rest, left):
        x, y, z = cell
        feat = jnp.concatenate(split3(weight_of(fields, spot, size_ref[index][1:2])), axis=0)
        feat = product_nt(rest.astype(jnp.bfloat16), feat.astype(jnp.bfloat16))
        feat = feat.astype(jnp.bfloat16)
        total = jnp.zeros((16, 24), jnp.float32)
        for dx in range(3):
            for dy in range(3):
                line = (x + dx) * ny + y + dy
                lanes = pl.ds(pl.multiple_of(z * 128, 128), 384)
                high, low = profile(product(left, flat_ref[line, :, lanes]))
                for dz in range(3):
                    cols = col_ref[line, pl.ds(pl.multiple_of((z + dz) * 256, 256), 256), :]
                    part = slice(dz * 128, (dz + 1) * 128)
                    pair = jnp.concatenate([high[:, part], low[:, part]], axis=1)
                    total += product(pair, cols)
                their_ref[line, :, lanes] += product_tn(feat, high) + product_tn(feat, low)
        sum_ref[index] += unsort(total, rest)

    placed = []
    for index, cell in enumerate(cells):
        fields = src_ref[cell[0] + 1, cell[1] + 1, cell[2] + 1]
        origin = origin_of([c + 1 for c in cell], sizes)
        placed.append((fields, origin))
        spot, square = place(fields, origin)
        set_rows(index, cell, fields, spot, square, size_ref[index][0:1], None)

    far_ref[...] = jnp.zeros_like(far_ref)
    close_ref[...] = jnp.zeros_like(close_ref)
    for x, y, z in cells_of(sizes):
        runs = source_runs((x, y, z), local, 16)
        line = x * ny + y
        part = slice(z * 128, (z + 1) * 128)
        left = rows_of(left_ref, runs)
        s = product(left, dens_ref[line, :, part])
        a, b = spline(s, tiled(root_ref[line, :, part], left.shape[0] // 8))
        add_rows(far_ref, runs, a)
        add_rows(close_ref, runs, b)

    for index, cell in enumerate(cells):
        part = slice(inner + index * WIDE, inner + index * WIDE + 16)
        octant = gather_rows(
            lambda start: 2.0 * far_ref[start : start + 32, :] - close_ref[start : start + 32, :],
            cell,
            halves,
        )
        total = unsorted_column(index, octant, 2.0 * far_ref[part, :] - close_ref[part, :])
        sum_ref[index, 0:8, :] = jnp.broadcast_to(total, (8, 128))
    extras(extra_density, 1)
    for index, cell in enumerate(cells):
        x, y, z = cell
        fields, origin = placed[index]
        spot, square = place(fields, origin)
        inverse = 1.0 / size_ref[index][0:1]
        density = kernel_norm * sum_ref[index, 0:1, :] * (inverse * inverse * inverse)
        rho_ref[x, y, z : z + 1, :] = density
        length = eta_factor * cube_root(fields[3:4] / density)
        _, strength = smooth(fields, density)
        size_ref[index] = jnp.where(row == 0, length, strength)
        set_rows(index, cell, fields, spot, square, length, weight_of(fields, spot, strength))

    own_ref[...] = jnp.zeros_like(own_ref)

    sum_ref[...] = jnp.zeros_like(sum_ref)
    their_ref[...] = jnp.zeros_like(their_ref)

    def part_of(source):
        x, y, z = source
        return x * ny + y, slice(z * 128, (z + 1) * 128)

    def put(source, value):
        line, part = part_of(source)
        their_ref[line, :, part] = value

    def flat_of(source):
        line, part = part_of(source)
        return flat_ref[line, :, part]

    def cols_of(source):
        x, y, z = source
        return col_ref[x * ny + y, z * 256 : (z + 1) * 256, :]

    outer = [cell for cell in cells_of(sizes) if cell[2] in (0, nz - 1)]
    force_sums(outer, left_ref, feat_ref, own_ref, flat_of, cols_of, put, local)
    extras(extra_force, WIDE // 16)

    for x, y, z in cells_of(sizes):
        spot, square = place(src_ref[x, y, z], origin_of((x, y, z), sizes))
        their = their_ref[x * ny + y, :, z * 128 : (z + 1) * 128]
        their = their[0:8] + their[8:16] + their[16:24]
        their = (spot * their[3:4] - their)[0:4]
        if z == 0:
            low_ref[x, y, 0] = their
        elif z == nz - 1:
            high_ref[x, y, 0] = their
        else:
            inner_ref[x, y, z - 1] = their


def profile(s):
    s = jnp.maximum(s, TINY)
    rs = lax.rsqrt(s)
    q = s * rs
    t = 1.0 - q
    a = jnp.maximum(t, 0.0)
    b = jnp.maximum(t - q, 0.0)
    g = jnp.minimum(a, q) * (a + b) * rs
    high = g.astype(jnp.bfloat16)
    return high, (g - high.astype(jnp.float32)).astype(jnp.bfloat16)


def smooth(fields, density):
    inverse = 1.0 / (eta_factor * cube_root(fields[3:4] / density))
    inv2 = inverse * inverse
    press = (gamma_index - 1.0) * fields[7:8] / density
    return inv2, press * (-6.0 * kernel_norm) * inv2 * inv2 * inverse


def take(block, dim, start, stop):
    return lax.slice_in_dim(block, start, stop, axis=dim)


def fold(block, low, high, edges):
    for dim in (2, 1, 0):
        axis = AXES[dim]
        if dim < 2:
            last = block.shape[dim] - 1
            low = take(block, dim, 0, 1) + edges[dim][0]
            high = take(block, dim, last, last + 1) + edges[dim][1]
            block = take(block, dim, 1, last)
        if lax.axis_size(axis) == 2:
            both = move(jnp.concatenate([high, low], axis=dim), axis, 1)
            to_first, to_last = take(both, dim, 0, 1), take(both, dim, 1, 2)
        else:
            to_last = move(low, axis, -1)
            to_first = move(high, axis, 1)
        count = block.shape[dim]
        if count == 1:
            block = block + to_first + to_last
        else:
            block = jnp.concatenate(
                [
                    take(block, dim, 0, 1) + to_first,
                    take(block, dim, 1, count - 1),
                    take(block, dim, count - 1, count) + to_last,
                ],
                axis=dim,
            )
    return block


def body(offsets, masses, smoothing, velocity, energy, active):
    local = masses.shape[:3]
    sizes = tuple(n + 2 for n in local)
    nx, ny, nz = sizes
    f32 = jnp.float32
    bf16 = jnp.bfloat16
    ncell = local[0] * local[1] * local[2]
    static = jnp.stack(
        [offsets[0], offsets[1], offsets[2], masses, velocity[0], velocity[1], velocity[2], energy],
        axis=3,
    )
    side = pl.pallas_call(
        functools.partial(sort_kernel, local=local),
        out_shape=jax.ShapeDtypeStruct((ncell, 8, 128), f32),
        compiler_params=pltpu.CompilerParams(vmem_limit_bytes=VMEM_LIMIT),
        name="sort",
    )(static, active)
    wide = halo(static, (0,))

    def begin(block, crossing):
        lines = nx * (2 if crossing else local[1])
        return pl.pallas_call(
            functools.partial(early_kernel, sizes=sizes, crossing=crossing),
            out_shape=jax.ShapeDtypeStruct((ncell, 8, 128), f32),
            scratch_shapes=[
                pltpu.VMEM((lines, 48, local[2] * 128), bf16),
                pltpu.VMEM((lines, 8, local[2] * 128), f32),
            ],
            compiler_params=pltpu.CompilerParams(vmem_limit_bytes=VMEM_LIMIT),
        )(block, smoothing)

    early = begin(wide, False)
    tall = halo(wide, (1,))
    second = begin(tall, True)
    padded = halo(tall, (2,))
    lines = nx * ny
    rows = ncell * (128 + WIDE)
    density, inner, low, high, *kept = pl.pallas_call(
        functools.partial(main_kernel, sizes=sizes),
        out_shape=(
            jax.ShapeDtypeStruct(masses.shape, f32),
            jax.ShapeDtypeStruct((nx, ny, local[2], 4, 128), f32),
            jax.ShapeDtypeStruct((nx, ny, 1, 4, 128), f32),
            jax.ShapeDtypeStruct((nx, ny, 1, 4, 128), f32),
            jax.ShapeDtypeStruct((ncell, 8, 128), f32),
            jax.ShapeDtypeStruct((rows, 48), bf16),
            jax.ShapeDtypeStruct((rows, 24), bf16),
            jax.ShapeDtypeStruct((ncell, 128, 128), bf16),
            jax.ShapeDtypeStruct((ncell, 8, 128), f32),
            jax.ShapeDtypeStruct((rows, 24), f32),
            jax.ShapeDtypeStruct((ncell, 24, 128), f32),
        ),
        scratch_shapes=[
            pltpu.VMEM((lines, 48, nz * 128), bf16),
            pltpu.VMEM((lines, 8, nz * 128), f32),
            pltpu.VMEM((lines, 48, nz * 128), bf16),
            pltpu.VMEM((lines, nz * 256, 24), bf16),
            pltpu.VMEM((rows, 128), f32),
            pltpu.VMEM((rows, 128), f32),
            pltpu.VMEM((lines, 24, nz * 128), f32),
            pltpu.SMEM((ncell,), jnp.int32),
        ],
        compiler_params=pltpu.CompilerParams(vmem_limit_bytes=VMEM_LIMIT),
        name="main",
    )(padded, smoothing, side, early, second)

    def edge(dim):
        shape = [n if k < dim else n - 2 for k, n in enumerate(sizes)]
        shape[dim] = 1
        count = 2 * shape[0] * shape[1] * shape[2]
        side_shape = jax.ShapeDtypeStruct(tuple(shape) + (4, 128), f32)
        return pl.pallas_call(
            functools.partial(edge_kernel, sizes=sizes, dim=dim),
            out_shape=(jax.ShapeDtypeStruct((rows, 24), f32), side_shape, side_shape),
            scratch_shapes=[pltpu.VMEM((count, 48, 128), bf16), pltpu.VMEM((count, 256, 24), bf16)],
            compiler_params=pltpu.CompilerParams(vmem_limit_bytes=VMEM_LIMIT),
        )(padded, kept[1], kept[2])

    tall_own, *tall_edges = edge(1)
    wide_own, *wide_edges = edge(0)
    push, heat = pl.pallas_call(
        functools.partial(rest_kernel, sizes=sizes),
        out_shape=(
            jax.ShapeDtypeStruct(local + (4, 128), f32),
            jax.ShapeDtypeStruct(masses.shape, f32),
        ),
        scratch_shapes=[
            pltpu.VMEM((ncell, 48, 128), bf16),
            pltpu.VMEM((ncell, 256, 24), bf16),
            pltpu.VMEM((rows, 24), f32),
            pltpu.VMEM((ncell, 24, 128), f32),
        ],
        compiler_params=pltpu.CompilerParams(vmem_limit_bytes=VMEM_LIMIT),
        name="rest",
    )(static, side, *kept, wide_own, tall_own)
    edges = (wide_edges, tall_edges)
    total = -(push[..., 0:3, :] + fold(inner, low, high, edges)[..., 0:3, :]) * push[..., 3:4, :]
    return (density, jnp.moveaxis(total, 3, 0), heat)


def solution(mesh):
    vector = P(None, "gx", "gy", "gz", None)
    scalar = P("gx", "gy", "gz", None)
    return jax.shard_map(
        body,
        mesh=mesh,
        in_specs=(vector, scalar, scalar, vector, scalar, scalar),
        out_specs=(scalar, vector, scalar),
        check_vma=False,
    )
```

```python
import functools

import jax
import jax.numpy as jnp
from jax import lax
from jax.experimental import pallas as pl
from jax.experimental.pallas import tpu as pltpu
from jax.sharding import PartitionSpec as P


kernel_norm = 2.5464790894703255
eta_factor = 2.3
gamma_index = 5.0 / 3.0

ROWS = 32
TINY = 1e-12
WIDE = 32
VMEM_LIMIT = 24 * 1024 * 1024
AXES = ("gx", "gy", "gz")


def ring(axis, step):
    count = lax.axis_size(axis)
    return [(i, (i + step) % count) for i in range(count)]


def move(block, axis, step):
    return lax.ppermute(block, axis, ring(axis, step))


def halo(block, dims):
    for dim in dims:
        axis = AXES[dim]
        size = block.shape[dim]
        if lax.axis_size(axis) == 2:
            other = move(block, axis, 1)
            low = lax.slice_in_dim(other, size - 1, size, axis=dim)
            high = lax.slice_in_dim(other, 0, 1, axis=dim)
        else:
            low = lax.slice_in_dim(block, size - 1, size, axis=dim)
            low = move(low, axis, 1)
            high = move(lax.slice_in_dim(block, 0, 1, axis=dim), axis, -1)
        block = jnp.concatenate([low, block, high], axis=dim)
    return block


def cube_root(value):
    return jnp.exp(jnp.log(value) * (1.0 / 3.0))


def split3(value):
    high = value.astype(jnp.bfloat16).astype(jnp.float32)
    rest = value - high
    mid = rest.astype(jnp.bfloat16).astype(jnp.float32)
    return high, mid, rest - mid


def row_index():
    return lax.broadcasted_iota(jnp.int32, (8, 128), 0)


def place(fields, origin):
    row = row_index()
    shift = jnp.where(row == 0, origin[0], jnp.where(row == 1, origin[1], origin[2]))
    spot = jnp.where(row < 3, fields + shift, 0.0)
    return spot, jnp.sum(spot * spot, axis=0, keepdims=True)


def source_rows(spot, square, scale):
    row = row_index()
    value = jnp.where(row == 3, square, jnp.where(row == 4, 1.0, spot)) * scale
    high, mid, low = split3(value)
    return jnp.concatenate([high, mid, high, mid, low, high], axis=0)


def target_rows(spot, square, scale):
    row = row_index()
    value = jnp.where(row == 3, 1.0, jnp.where(row == 4, square, -2.0 * spot)) * scale
    high, mid, low = split3(value)
    return jnp.concatenate([high, high, mid, mid, high, low], axis=0)


def product(left, right):
    return jnp.dot(left, right, preferred_element_type=jnp.float32)


def product_nt(left, right):
    return lax.dot_general(
        left, right, (((1,), (1,)), ((), ())), preferred_element_type=jnp.float32
    )


def product_tn(left, right):
    return lax.dot_general(
        left, right, (((0,), (0,)), ((), ())), preferred_element_type=jnp.float32
    )


def tiled(rows, count):
    return jnp.concatenate([rows] * count, axis=0)


def origin_of(cell, sizes):
    return [c - 0.5 * n for c, n in zip(cell, sizes)]


def cells_of(sizes):
    return [(x, y, z) for x in range(sizes[0]) for y in range(sizes[1]) for z in range(sizes[2])]


def spline(s, root):
    s = jnp.maximum(s, TINY)
    scaled = s * lax.rsqrt(s)
    t = root - scaled
    a = jnp.maximum(t, 0.0)
    b = jnp.maximum(t - scaled, 0.0)
    return a * a * a, b * b * b


def dense_sums(left, dens_ref, root_ref, spans):
    count = left.shape[0]
    near = jnp.zeros((count, 128), jnp.float32)
    far = jnp.zeros((count, 128), jnp.float32)
    for line, lanes, cells in spans:
        s = product(left, dens_ref[line, :, lanes])
        a, b = spline(s, tiled(root_ref[line, :, lanes], count // 8))
        for k in range(cells):
            far = far + a[:, k * 128 : (k + 1) * 128]
            near = near + b[:, k * 128 : (k + 1) * 128]
    return 2.0 * far - near


def row_sums(left, dens_ref, root_ref, spans):
    sums = [
        dense_sums(left[k : k + ROWS], dens_ref, root_ref, spans) for k in range(0, 128, ROWS)
    ]
    return jnp.sum(jnp.concatenate(sums, axis=0).T, axis=0, keepdims=True)


def density_tables(dens_ref, root_ref, line, z, fields, spot, square):
    root = cube_root(fields[3:4])
    part = slice(z * 128, (z + 1) * 128)
    dens_ref[line, :, part] = source_rows(spot, square, root * root).astype(jnp.bfloat16)
    root_ref[line, :, part] = jnp.broadcast_to(root, (8, 128))


def lane_runs(cells, first):
    runs = []
    for z in cells:
        if runs and runs[-1][1] == z:
            runs[-1][1] = z + 1
        else:
            runs.append([z, z + 1])
    return [(slice((a - first) * 128, (b - first) * 128), b - a) for a, b in runs]


def early_kernel(src_ref, len_ref, sum_ref, dens_ref, root_ref, *, sizes, crossing):
    nx, ny, nz = sizes
    cx, cy, cz = nx - 2, ny - 2, nz - 2
    columns = (0, ny - 1) if crossing else tuple(range(1, ny - 1))
    shift = 0 if crossing else 1
    for x, y, z in cells_of((nx, len(columns), cz)):
        fields = src_ref[x, columns[y] - shift, z]
        spot, square = place(fields, origin_of((x, columns[y], z + 1), sizes))
        density_tables(dens_ref, root_ref, x * len(columns) + y, z, fields, spot, square)

    def one_plane(x, carry):
        for y in range(cy):
            for z in range(cz):
                fields = src_ref[x + 1, y + 1 - shift, z]
                where = [x.astype(jnp.float32) + (1.0 - 0.5 * nx)]
                where += [y + 1.0 - 0.5 * ny, z + 1.0 - 0.5 * nz]
                spot, square = place(fields, where)
                inverse = 1.0 / len_ref[x, y, z : z + 1, :]
                left = target_rows(spot, square, inverse * inverse).T.astype(jnp.bfloat16)
                spans = []
                for dx in range(3):
                    for at, source in enumerate(columns):
                        if abs(source - y - 1) <= 1:
                            for lanes, cells in lane_runs(near_of(z + 1, cz), 0):
                                spans.append(((x + dx) * len(columns) + at, lanes, cells))
                total = jnp.zeros((1, 128), jnp.float32)
                if spans:
                    total = row_sums(left, dens_ref, root_ref, spans)
                sum_ref[(x * cy + y) * cz + z] = jnp.broadcast_to(total, (8, 128))
        return carry

    lax.fori_loop(0, cx, one_plane, 0)


def half_up(count):
    return jnp.floor((count + 1.0) * 0.5)


def sort_kernel(src_ref, act_ref, side_ref, *, local):
    row = row_index()
    across = lax.broadcasted_iota(jnp.int32, (128, 128), 0)
    along = lax.broadcasted_iota(jnp.int32, (128, 128), 1)
    earlier = across < along

    def rank(key):
        left = jnp.broadcast_to(key, (8, 128)).T[:, 0:1]
        ahead = (left < key) | (earlier & (left == key))
        return jnp.sum(jnp.where(ahead, 1.0, 0.0), axis=0, keepdims=True)

    for index, cell in enumerate(cells_of(local)):
        fields = src_ref[cell]
        mass = fields[3:4]
        heavy = jnp.where(mass > jnp.sum(mass, axis=1, keepdims=True) * (1.0 / 128.0), 1.0, 0.0)
        light = 128.0 - jnp.sum(heavy, axis=1, keepdims=True)
        base = jnp.zeros((1, 128), jnp.float32)
        size = jnp.broadcast_to(light, (1, 128))
        group = jnp.zeros((1, 128), jnp.float32)
        bits = []
        for dim in range(3):
            place_in = rank(fields[dim : dim + 1] + 2.0 * group + 64.0 * heavy) - base
            first = half_up(size)
            bit = jnp.where(place_in >= first, 1.0, 0.0) * (1.0 - heavy)
            base = base + bit * first
            size = jnp.where(bit > 0.0, size - first, first)
            group = 2.0 * group + bit
            place_in = place_in - bit * first
            bits.append(bit)
        slot = jnp.where(heavy > 0.0, -1.0, 16.0 * group + place_in)
        side = jnp.where(row == 0, bits[0], jnp.where(row == 1, bits[1], bits[2]))
        side = jnp.where(row == 3, heavy, side)
        side = jnp.where(row == 4, slot, side)
        x, y, z = cell
        active = act_ref[x, y, z : z + 1, :].astype(jnp.float32)
        side_ref[index] = jnp.where(row == 5, active, side)


def halves_of(source, count):
    reach = []
    for half in range(2 * count):
        cell = half // 2 + 1
        if source in ((cell - 1, cell) if half % 2 == 0 else (cell, cell + 1)):
            reach.append(half)
    return reach


def near_of(source, count):
    return [c for c in range(count) if abs(c + 1 - source) <= 1]


def runs_of(ranges, counts):
    xs, ys, zs = ranges
    return [
        (((x * counts[1] + y) * counts[2] + zs[0]) * 16, len(zs) * 16) for x in xs for y in ys
    ]


def cell_runs(cell, halves):
    x, y, z = cell
    return [
        (((2 * x + bx) * halves[1] + 2 * y + by) * halves[2] + 2 * z) * 16
        for bx in range(2)
        for by in range(2)
    ]


def scatter_rows(ref, cell, halves, value):
    for k, start in enumerate(cell_runs(cell, halves)):
        ref[start : start + 32, :] = value[k * 32 : (k + 1) * 32]


def gather_rows(value_of, cell, halves):
    return jnp.concatenate([value_of(start) for start in cell_runs(cell, halves)], axis=0)


def source_runs(source, local, count):
    inner = 128 * local[0] * local[1] * local[2]
    ranges = [halves_of(s, n) for s, n in zip(source, local)]
    runs = runs_of(ranges, [2 * n for n in local])
    ranges = [near_of(s, n) for s, n in zip(source, local)]
    for start, size in runs_of(ranges, local):
        for first in range(start // 16, (start + size) // 16):
            runs.append((inner + first * WIDE, count))
    return runs


def rows_of(ref, runs):
    return jnp.concatenate([ref[start : start + size, :] for start, size in runs], axis=0)


def add_rows(ref, runs, value):
    at = 0
    for start, size in runs:
        ref[start : start + size, :] += value[at : at + size]
        at += size


def picked(rest_ref, index, first, count):
    order = rest_ref[index][0:1] - first
    slots = lax.broadcasted_iota(jnp.int32, (count, 128), 0).astype(jnp.float32)
    return jnp.where(slots == order, 1.0, 0.0)


def unsort(value, rest):
    pieces = split3(value)
    rest = rest.astype(jnp.bfloat16)
    total = product_tn(pieces[0].astype(jnp.bfloat16), rest)
    total += product_tn(pieces[1].astype(jnp.bfloat16), rest)
    return total + product_tn(pieces[2].astype(jnp.bfloat16), rest)


def force_columns(fields, spot):
    row = row_index()
    moving = jnp.sum(fields[4:7] * spot[0:3], axis=0, keepdims=True)
    basis = jnp.where(row < 3, spot, jnp.where(row == 3, 1.0, fields))
    basis = jnp.where(row == 7, moving, basis) * fields[3:4]
    return jnp.concatenate(split3(basis), axis=0).T.astype(jnp.bfloat16)


def force_sums(sources, left_ref, feat_ref, own_ref, flat_of, cols_of, put, local):
    def sums(source, runs, high, low):
        add_rows(own_ref, runs, product(jnp.concatenate([high, low], axis=1), cols_of(source)))
        feat = rows_of(feat_ref, runs)
        put(source, product_tn(feat, high) + product_tn(feat, low))

    waiting = None
    for source in sources:
        runs = source_runs(source, local, WIDE)
        high, low = profile(product(rows_of(left_ref, runs), flat_of(source)))
        if waiting is not None:
            sums(*waiting)
        waiting = (source, runs, high, low)
    sums(*waiting)


def is_local(cell, local):
    return all(0 < c <= n for c, n in zip(cell, local))


def rest_kernel(
    src_ref,
    side_ref,
    size_ref,
    left_ref,
    feat_ref,
    oct_ref,
    rest_ref,
    part_ref,
    sum_ref,
    push_ref,
    heat_ref,
    flat_ref,
    col_ref,
    own_ref,
    their_ref,
    *,
    sizes,
):
    local = tuple(n - 2 for n in sizes)
    halves = [2 * n for n in local]
    cells = cells_of(local)
    inner = 128 * len(cells)
    numbers = {tuple(c + 1 for c in cell): k for k, cell in enumerate(cells)}
    places = []
    for index, cell in enumerate(cells):
        fields = src_ref[cell]
        spot, square = place(fields, origin_of([c + 1 for c in cell], sizes))
        flat_ref[index] = source_rows(spot, square, 1.0).astype(jnp.bfloat16)
        cols = force_columns(fields, spot)
        col_ref[index, 0:128, :] = cols
        col_ref[index, 128:256, :] = cols
        places.append((fields, spot[0:3]))
    own_ref[...] = part_ref[...]

    def put(source, value):
        their_ref[numbers[source]] = value

    force_sums(
        list(numbers),
        left_ref,
        feat_ref,
        own_ref,
        lambda source: flat_ref[numbers[source]],
        lambda source: col_ref[numbers[source]],
        put,
        local,
    )
    for index, cell in enumerate(cells):
        fields, spot = places[index]
        octant = gather_rows(lambda start: own_ref[start : start + 32, :], cell, halves)
        part = slice(inner + index * WIDE, inner + index * WIDE + WIDE)
        own = unsort(octant, oct_ref[index]) + sum_ref[index]
        own += unsort(own_ref[part, :], picked(rest_ref, index, 0.0, WIDE))
        own = (own[0:8] + own[8:16] + own[16:24]) * size_ref[index][1:2]
        their = their_ref[index]
        their = their[0:8] + their[8:16] + their[16:24]
        active = side_ref[index, 5:6, :]
        push = spot * own[3:4] - own[0:3]
        heat = fields[4:7] * push - spot * own[4:7]
        heat = jnp.sum(heat, axis=0, keepdims=True) + own[7:8]
        push = push + spot * their[3:4] - their[0:3]
        push_ref[cell] = jnp.concatenate([push, active], axis=0)
        heat_ref[cell[0], cell[1], cell[2] : cell[2] + 1, :] = active * heat


def main_kernel(
    src_ref,
    len_ref,
    side_ref,
    early_ref,
    second_ref,
    rho_ref,
    inner_ref,
    low_ref,
    high_ref,
    size_ref,
    left_ref,
    feat_ref,
    oct_ref,
    rest_ref,
    own_ref,
    sum_ref,
    dens_ref,
    root_ref,
    flat_ref,
    col_ref,
    far_ref,
    close_ref,
    their_ref,
    count_ref,
    *,
    sizes,
):
    nx, ny, nz = sizes
    local = cx, cy, cz = nx - 2, ny - 2, nz - 2
    halves = (2 * cx, 2 * cy, 2 * cz)
    cells = cells_of(local)
    inner = len(cells) * 128
    row = row_index()
    across = lax.broadcasted_iota(jnp.int32, (128, 128), 0)
    along = lax.broadcasted_iota(jnp.int32, (128, 128), 1)
    before = jnp.where(across < along, 1.0, 0.0).astype(jnp.bfloat16)
    slot_of = across.astype(jnp.float32)

    for x, y, z in cells_of(sizes):
        fields = src_ref[x, y, z]
        spot, square = place(fields, origin_of((x, y, z), sizes))
        line = x * ny + y
        part = slice(z * 128, (z + 1) * 128)
        density_tables(dens_ref, root_ref, line, z, fields, spot, square)
        flat_ref[line, :, part] = source_rows(spot, square, 1.0).astype(jnp.bfloat16)
        cols = force_columns(fields, spot)
        col_ref[line, z * 256 : z * 256 + 128, :] = cols
        col_ref[line, z * 256 + 128 : z * 256 + 256, :] = cols

    def first_pass(x, carry):
        for y in range(cy):
            for z in range(cz):
                index = (x * cy + y) * cz + z
                fields = src_ref[x + 1, y + 1, z + 1]
                where = [x.astype(jnp.float32) + (1.0 - 0.5 * nx)]
                where += [y + 1.0 - 0.5 * ny, z + 1.0 - 0.5 * nz]
                spot, square = place(fields, where)
                inverse = 1.0 / len_ref[x, y, z : z + 1, :]
                left = target_rows(spot, square, inverse * inverse).T.astype(jnp.bfloat16)
                spans = []
                for dx in range(3):
                    for source in range(y, y + 3):
                        known = [c + 1 for c in near_of(z + 1, cz)]
                        rest = [c for c in range(z, z + 3) if c not in known]
                        for lanes, cells in lane_runs(rest, 0):
                            spans.append(((x + dx) * ny + source, lanes, cells))
                total = early_ref[index][0:1] + second_ref[index][0:1]
                if spans:
                    total += row_sums(left, dens_ref, root_ref, spans)
                density = kernel_norm * total * (inverse * inverse * inverse)
                length = eta_factor * cube_root(fields[3:4] / density)
                size_ref[index] = jnp.broadcast_to(length, (8, 128))
        return carry

    lax.fori_loop(0, cx, first_pass, 0)

    def choose(index, fields, length):
        side = side_ref[index]
        reach = jnp.where(side > 0.0, length - fields, fields + length - 1.0)
        wide = jnp.where((row < 3) & (reach > 0.0), 1.0, 0.0)
        wide = jnp.where(row == 3, side, wide)
        wide = jnp.max(wide, axis=0, keepdims=True)
        order = product(jnp.broadcast_to(wide, (8, 128)).astype(jnp.bfloat16), before)[0:1]
        order = jnp.where(wide > 0.0, order, -1.0)
        count_ref[index] = jnp.sum(wide).astype(jnp.int32)
        slot = jnp.where(wide > 0.0, -1.0, side[4:5])
        oct_ref[index] = jnp.where(slot_of == slot, 1.0, 0.0).astype(jnp.bfloat16)
        rest_ref[index] = jnp.broadcast_to(order, (8, 128))

    def set_rows(index, cell, fields, spot, square, length, weight):
        inverse = 1.0 / length
        choose(index, fields, length)
        count = 16 if weight is None else WIDE
        rest = picked(rest_ref, index, 0.0, count).astype(jnp.bfloat16)
        left = target_rows(spot, square, inverse * inverse).astype(jnp.bfloat16)
        chosen = oct_ref[index]
        scatter_rows(left_ref, cell, halves, product_nt(chosen, left).astype(jnp.bfloat16))
        part = slice(inner + index * WIDE, inner + index * WIDE + count)
        left_ref[part, :] = product_nt(rest, left).astype(jnp.bfloat16)
        if weight is not None:
            feat = jnp.concatenate(split3(weight), axis=0).astype(jnp.bfloat16)
            scatter_rows(feat_ref, cell, halves, product_nt(chosen, feat).astype(jnp.bfloat16))
            feat_ref[part, :] = product_nt(rest, feat).astype(jnp.bfloat16)

    def unsorted_column(index, octant, rest):
        total = jnp.sum(octant, axis=1, keepdims=True) * oct_ref[index].astype(jnp.float32)
        total = jnp.sum(total, axis=0, keepdims=True)
        rest = jnp.sum(rest, axis=1, keepdims=True) * picked(rest_ref, index, 0.0, 16)
        return total + jnp.sum(rest, axis=0, keepdims=True)

    def extras(visit, first):
        def one_cell(index, carry):
            def one_chunk(chunk, carry):
                x = index // (cy * cz)
                y = index // cz % cy
                z = index % cz
                fields = src_ref[x + 1, y + 1, z + 1]
                where = [v.astype(jnp.float32) + (1.0 - 0.5 * n) for v, n in zip((x, y, z), sizes)]
                spot, square = place(fields, where)
                inverse = 1.0 / size_ref[index][0:1]
                rest = picked(rest_ref, index, chunk.astype(jnp.float32) * 16.0, 16)
                left = target_rows(spot, square, inverse * inverse).astype(jnp.bfloat16)
                left = product_nt(rest.astype(jnp.bfloat16), left).astype(jnp.bfloat16)
                visit(index, (x, y, z), fields, spot, rest, left)
                return carry

            return lax.fori_loop(first, (count_ref[index] + 15) // 16, one_chunk, carry)

        lax.fori_loop(0, cx * cy * cz, one_cell, 0)

    def weight_of(fields, spot, strength):
        return jnp.where(row < 3, spot, jnp.where(row == 3, 1.0, 0.0)) * (fields[3:4] * strength)

    def extra_density(index, cell, fields, spot, rest, left):
        x, y, z = cell
        lanes = pl.ds(pl.multiple_of(z * 128, 128), 384)
        spans = [((x + dx) * ny + y + dy, lanes, 3) for dx in range(3) for dy in range(3)]
        extra = dense_sums(left, dens_ref, root_ref, spans)
        extra = jnp.sum(extra, axis=1, keepdims=True) * rest
        sum_ref[index, 0:8, :] += jnp.sum(extra, axis=0, keepdims=True)

    def extra_force(index, cell, fields, spot, rest, left):
        x, y, z = cell
        feat = jnp.concatenate(split3(weight_of(fields, spot, size_ref[index][1:2])), axis=0)
        feat = product_nt(rest.astype(jnp.bfloat16), feat.astype(jnp.bfloat16))
        feat = feat.astype(jnp.bfloat16)
        total = jnp.zeros((16, 24), jnp.float32)
        for dx in range(3):
            for dy in range(3):
                line = (x + dx) * ny + y + dy
                lanes = pl.ds(pl.multiple_of(z * 128, 128), 384)
                high, low = profile(product(left, flat_ref[line, :, lanes]))
                for dz in range(3):
                    cols = col_ref[line, pl.ds(pl.multiple_of((z + dz) * 256, 256), 256), :]
                    part = slice(dz * 128, (dz + 1) * 128)
                    pair = jnp.concatenate([high[:, part], low[:, part]], axis=1)
                    total += product(pair, cols)
                their_ref[line, :, lanes] += product_tn(feat, high) + product_tn(feat, low)
        sum_ref[index] += unsort(total, rest)

    placed = []
    for index, cell in enumerate(cells):
        fields = src_ref[cell[0] + 1, cell[1] + 1, cell[2] + 1]
        origin = origin_of([c + 1 for c in cell], sizes)
        placed.append((fields, origin))
        spot, square = place(fields, origin)
        set_rows(index, cell, fields, spot, square, size_ref[index][0:1], None)

    far_ref[...] = jnp.zeros_like(far_ref)
    close_ref[...] = jnp.zeros_like(close_ref)
    for x, y, z in cells_of(sizes):
        runs = source_runs((x, y, z), local, 16)
        line = x * ny + y
        part = slice(z * 128, (z + 1) * 128)
        left = rows_of(left_ref, runs)
        s = product(left, dens_ref[line, :, part])
        a, b = spline(s, tiled(root_ref[line, :, part], left.shape[0] // 8))
        add_rows(far_ref, runs, a)
        add_rows(close_ref, runs, b)

    for index, cell in enumerate(cells):
        part = slice(inner + index * WIDE, inner + index * WIDE + 16)
        octant = gather_rows(
            lambda start: 2.0 * far_ref[start : start + 32, :] - close_ref[start : start + 32, :],
            cell,
            halves,
        )
        total = unsorted_column(index, octant, 2.0 * far_ref[part, :] - close_ref[part, :])
        sum_ref[index, 0:8, :] = jnp.broadcast_to(total, (8, 128))
    extras(extra_density, 1)
    for index, cell in enumerate(cells):
        x, y, z = cell
        fields, origin = placed[index]
        spot, square = place(fields, origin)
        inverse = 1.0 / size_ref[index][0:1]
        density = kernel_norm * sum_ref[index, 0:1, :] * (inverse * inverse * inverse)
        rho_ref[x, y, z : z + 1, :] = density
        length = eta_factor * cube_root(fields[3:4] / density)
        _, strength = smooth(fields, density)
        size_ref[index] = jnp.where(row == 0, length, strength)
        set_rows(index, cell, fields, spot, square, length, weight_of(fields, spot, strength))

    own_ref[...] = jnp.zeros_like(own_ref)

    for index, cell in enumerate(cells):
        sum_ref[index] = jnp.zeros((24, 128), jnp.float32)
        x, y, z = [c + 1 for c in cell]
        their_ref[x * ny + y, :, z * 128 : (z + 1) * 128] = jnp.zeros((24, 128), jnp.float32)

    def part_of(source):
        x, y, z = source
        return x * ny + y, slice(z * 128, (z + 1) * 128)

    def put(source, value):
        line, part = part_of(source)
        their_ref[line, :, part] = value

    def flat_of(source):
        line, part = part_of(source)
        return flat_ref[line, :, part]

    def cols_of(source):
        x, y, z = source
        return col_ref[x * ny + y, z * 256 : (z + 1) * 256, :]

    outer = [cell for cell in cells_of(sizes) if not is_local(cell, local)]
    force_sums(outer, left_ref, feat_ref, own_ref, flat_of, cols_of, put, local)
    extras(extra_force, WIDE // 16)

    for x, y, z in cells_of(sizes):
        spot, square = place(src_ref[x, y, z], origin_of((x, y, z), sizes))
        their = their_ref[x * ny + y, :, z * 128 : (z + 1) * 128]
        their = their[0:8] + their[8:16] + their[16:24]
        their = (spot * their[3:4] - their)[0:4]
        if z == 0:
            low_ref[x, y, 0] = their
        elif z == nz - 1:
            high_ref[x, y, 0] = their
        else:
            inner_ref[x, y, z - 1] = their


def profile(s):
    s = jnp.maximum(s, TINY)
    rs = lax.rsqrt(s)
    q = s * rs
    t = 1.0 - q
    a = jnp.maximum(t, 0.0)
    b = jnp.maximum(t - q, 0.0)
    g = jnp.minimum(a, q) * (a + b) * rs
    high = g.astype(jnp.bfloat16)
    return high, (g - high.astype(jnp.float32)).astype(jnp.bfloat16)


def smooth(fields, density):
    inverse = 1.0 / (eta_factor * cube_root(fields[3:4] / density))
    inv2 = inverse * inverse
    press = (gamma_index - 1.0) * fields[7:8] / density
    return inv2, press * (-6.0 * kernel_norm) * inv2 * inv2 * inverse


def take(block, dim, start, stop):
    return lax.slice_in_dim(block, start, stop, axis=dim)


def fold(block, low, high):
    for dim in (2, 1, 0):
        axis = AXES[dim]
        if dim < 2:
            last = block.shape[dim] - 1
            low, high = take(block, dim, 0, 1), take(block, dim, last, last + 1)
            block = take(block, dim, 1, last)
        if lax.axis_size(axis) == 2:
            both = move(jnp.concatenate([high, low], axis=dim), axis, 1)
            to_first, to_last = take(both, dim, 0, 1), take(both, dim, 1, 2)
        else:
            to_last = move(low, axis, -1)
            to_first = move(high, axis, 1)
        count = block.shape[dim]
        if count == 1:
            block = block + to_first + to_last
        else:
            block = jnp.concatenate(
                [
                    take(block, dim, 0, 1) + to_first,
                    take(block, dim, 1, count - 1),
                    take(block, dim, count - 1, count) + to_last,
                ],
                axis=dim,
            )
    return block


def body(offsets, masses, smoothing, velocity, energy, active):
    local = masses.shape[:3]
    sizes = tuple(n + 2 for n in local)
    nx, ny, nz = sizes
    f32 = jnp.float32
    bf16 = jnp.bfloat16
    ncell = local[0] * local[1] * local[2]
    static = jnp.stack(
        [offsets[0], offsets[1], offsets[2], masses, velocity[0], velocity[1], velocity[2], energy],
        axis=3,
    )
    side = pl.pallas_call(
        functools.partial(sort_kernel, local=local),
        out_shape=jax.ShapeDtypeStruct((ncell, 8, 128), f32),
        compiler_params=pltpu.CompilerParams(vmem_limit_bytes=VMEM_LIMIT),
        name="sort",
    )(static, active)
    wide = halo(static, (0,))

    def begin(block, crossing):
        lines = nx * (2 if crossing else local[1])
        return pl.pallas_call(
            functools.partial(early_kernel, sizes=sizes, crossing=crossing),
            out_shape=jax.ShapeDtypeStruct((ncell, 8, 128), f32),
            scratch_shapes=[
                pltpu.VMEM((lines, 48, local[2] * 128), bf16),
                pltpu.VMEM((lines, 8, local[2] * 128), f32),
            ],
            compiler_params=pltpu.CompilerParams(vmem_limit_bytes=VMEM_LIMIT),
        )(block, smoothing)

    early = begin(wide, False)
    tall = halo(wide, (1,))
    second = begin(tall, True)
    padded = halo(tall, (2,))
    lines = nx * ny
    rows = ncell * (128 + WIDE)
    density, inner, low, high, *kept = pl.pallas_call(
        functools.partial(main_kernel, sizes=sizes),
        out_shape=(
            jax.ShapeDtypeStruct(masses.shape, f32),
            jax.ShapeDtypeStruct((nx, ny, local[2], 4, 128), f32),
            jax.ShapeDtypeStruct((nx, ny, 1, 4, 128), f32),
            jax.ShapeDtypeStruct((nx, ny, 1, 4, 128), f32),
            jax.ShapeDtypeStruct((ncell, 8, 128), f32),
            jax.ShapeDtypeStruct((rows, 48), bf16),
            jax.ShapeDtypeStruct((rows, 24), bf16),
            jax.ShapeDtypeStruct((ncell, 128, 128), bf16),
            jax.ShapeDtypeStruct((ncell, 8, 128), f32),
            jax.ShapeDtypeStruct((rows, 24), f32),
            jax.ShapeDtypeStruct((ncell, 24, 128), f32),
        ),
        scratch_shapes=[
            pltpu.VMEM((lines, 48, nz * 128), bf16),
            pltpu.VMEM((lines, 8, nz * 128), f32),
            pltpu.VMEM((lines, 48, nz * 128), bf16),
            pltpu.VMEM((lines, nz * 256, 24), bf16),
            pltpu.VMEM((rows, 128), f32),
            pltpu.VMEM((rows, 128), f32),
            pltpu.VMEM((lines, 24, nz * 128), f32),
            pltpu.SMEM((ncell,), jnp.int32),
        ],
        compiler_params=pltpu.CompilerParams(vmem_limit_bytes=VMEM_LIMIT),
        name="main",
    )(padded, smoothing, side, early, second)
    push, heat = pl.pallas_call(
        functools.partial(rest_kernel, sizes=sizes),
        out_shape=(
            jax.ShapeDtypeStruct(local + (4, 128), f32),
            jax.ShapeDtypeStruct(masses.shape, f32),
        ),
        scratch_shapes=[
            pltpu.VMEM((ncell, 48, 128), bf16),
            pltpu.VMEM((ncell, 256, 24), bf16),
            pltpu.VMEM((rows, 24), f32),
            pltpu.VMEM((ncell, 24, 128), f32),
        ],
        compiler_params=pltpu.CompilerParams(vmem_limit_bytes=VMEM_LIMIT),
        name="rest",
    )(static, side, *kept)
    total = -(push[..., 0:3, :] + fold(inner, low, high)[..., 0:3, :]) * push[..., 3:4, :]
    return (density, jnp.moveaxis(total, 3, 0), heat)


def solution(mesh):
    vector = P(None, "gx", "gy", "gz", None)
    scalar = P("gx", "gy", "gz", None)
    return jax.shard_map(
        body,
        mesh=mesh,
        in_specs=(vector, scalar, scalar, vector, scalar, scalar),
        out_specs=(scalar, vector, scalar),
        check_vma=False,
    )
```
